256 devices in a mesh: lat: 16 (over z, core), rad: 16 (over x, y).
Axes of the slice: x: 4, y: 4, z: 8, core: 2. Of those that a mesh axis runs over, the one named last changes fastest.
Arguments:
- residual: float32 [3, 128, 128, 256], P(None, 'rad', 'lat'), may hold values from -30 to 30
- prev_basis: float32 [4, 3, 128, 128, 256], P(None, None, 'rad', 'lat'), may hold values from -30 to 30
- layer_ids: int32 [64, 64, 128], P('rad', 'lat'), may hold values from 0 to 7
- viscosity: float32 [8], replicated, may hold values from 0.1 to 1
- shifts: float32 [4], replicated, may hold values from 0.3 to 2
Outputs:
- new_basis: float32 [4, 3, 128, 128, 256], P(None, None, 'rad', 'lat')
- gram_matrix: float32 [9, 9], replicated
The draws below stay inside these ranges and needn't reach their ends.
All inputs are finite; a program needn't handle non-finite values.
Results may differ from the reference program's by a relative error of at most 0.00019.
Values sent between devices are 32-bit elements; how exact they have to be, the bound alone decides.
A program may use at most 128 MiB of HBM per device.

```python
import math
import jax
import jax.numpy as jnp
from jax import lax

COMP = 3
S = 4
PREV = 4
LAYERS = 8
ER = 4
EY = 128
BASIS = 9
NRE = 64
NXE = 64
NRN = 128
NXN = 128
NYN = 256
N_RAD = 16


def ramp_field(key, leading):
    full_shape = (leading, COMP, NRN, NXN, NYN)
    radial = (jnp.arange(NRN, dtype=jnp.float32) / NRN)[:, None, None]
    lateral = (jnp.arange(NXN, dtype=jnp.float32) / NXN)[None, :, None]
    across = (jnp.arange(NYN, dtype=jnp.float32) / NYN)[None, None, :]
    smooth = jnp.sin(6.0 * radial + 4.0 * lateral + 3.0 * across + 0.5)
    coef_key = jax.random.fold_in(key, 7)
    coefs = jax.random.truncated_normal(coef_key, -2.0, 2.0, (leading, COMP, 1, 1, 1), jnp.float32)
    noise_vals = jax.random.truncated_normal(key, -4.0, 4.0, full_shape, jnp.float32)
    amplitude = 3.0 ** (radial + lateral - 1.0)
    return (amplitude * (noise_vals + coefs * smooth)).astype(jnp.float32)


def draw_residual(key, part):
    return ramp_field(jax.random.fold_in(key, 11), 1)[0]


def draw_prev_basis(key, part):
    return ramp_field(jax.random.fold_in(key, 23), PREV)


def touch_ends(values, stream_key, low, largest):
    spot = [jax.random.randint(jax.random.fold_in(stream_key, axis), (), 0, length) for axis, length in enumerate(values.shape)]
    widest = values.shape.index(max(values.shape))
    beside = spot[:widest] + [(spot[widest] + 1) % values.shape[widest]] + spot[widest + 1:]
    return values.at[tuple(spot)].set(low).at[tuple(beside)].set(largest)


def setup_inputs(seed: int = 0) -> dict:
    splits = jax.random.split(jax.random.key(seed), 6)
    residual = draw_residual(jax.random.fold_in(splits[5], 71), 0)
    prev_basis = draw_prev_basis(jax.random.fold_in(splits[5], 71), 0)
    layer_ids = touch_ends(jax.random.randint(splits[2], (NRE, NXE, EY), 0, LAYERS), jax.random.fold_in(splits[2], 1), 0, LAYERS - 1).astype(jnp.int32)
    viscosity = jnp.clip(jnp.exp(jax.random.uniform(splits[3], (LAYERS,), jnp.float32, math.log(0.1), math.log(1.0))), 0.1, 1.0)
    shifts = jnp.clip(jax.random.uniform(splits[4], (S,), jnp.float32, 0.3, 2.0), 0.3, 2.0)
    return {"residual": residual, "prev_basis": prev_basis, "layer_ids": layer_ids, "viscosity": viscosity, "shifts": shifts}


stiff_line = ((7.0 / 3, -8.0 / 3, 1.0 / 3), (-8.0 / 3, 16.0 / 3, -8.0 / 3), (1.0 / 3, -8.0 / 3, 7.0 / 3))
mass_line = ((4.0 / 30, 2.0 / 30, -1.0 / 30), (2.0 / 30, 16.0 / 30, 2.0 / 30), (-1.0 / 30, 2.0 / 30, 4.0 / 30))


def contract(line_table, element_vals, axis_pos):
    pieces = [lax.index_in_dim(element_vals, j, axis_pos, keepdims=False) for j in range(3)]
    row_terms = [line_table[i][0] * pieces[0] + line_table[i][1] * pieces[1] + line_table[i][2] * pieces[2] for i in range(3)]
    return jnp.stack(row_terms, axis_pos)


def split_local(field_in, axis_pos):
    el_count = field_in.shape[axis_pos] // 2 - 1
    return jnp.stack([lax.slice_in_dim(field_in, k, k + 2 * el_count - 1, 2, axis_pos) for k in range(3)], 0)


def join_local(element_vals, axis_pos):
    lower_side = element_vals[0]
    middle = element_vals[1]
    upper_side = element_vals[2]
    el_count = lower_side.shape[axis_pos]
    even_nodes = lax.slice_in_dim(lower_side, 1, el_count, 1, axis_pos) + lax.slice_in_dim(upper_side, 0, el_count - 1, 1, axis_pos)
    odd_nodes = lax.slice_in_dim(middle, 1, el_count, 1, axis_pos)
    alternated = jnp.stack([even_nodes, odd_nodes], axis_pos + 1)
    new_shape = list(even_nodes.shape)
    new_shape[axis_pos] = 2 * (el_count - 1)
    return alternated.reshape(new_shape)


def stiffness(field_in, viscous):
    padded = jnp.pad(field_in, ((0, 0), (0, 0), (0, 0), (2, 2)))
    element_vals = split_local(padded, 1)
    element_vals = split_local(element_vals, 3)
    element_vals = split_local(element_vals, 5)
    along_y = contract(mass_line, element_vals, 0)
    mass_rx = contract(mass_line, along_y, 1)
    term_r = contract(stiff_line, mass_rx, 2)
    term_x = contract(mass_line, contract(stiff_line, along_y, 1), 2)
    term_y = contract(stiff_line, contract(mass_line, contract(mass_line, element_vals, 2), 1), 0)
    viscous_wide = jnp.pad(viscous, ((0, 0), (0, 0), (1, 0)))
    weighted = (term_r + term_x + term_y) * viscous_wide
    assembled = join_local(weighted, 5)
    assembled = join_local(assembled, 3)
    return join_local(assembled, 1)


def reference(residual, prev_basis, layer_ids, viscosity, shifts):
    viscous = jnp.take(viscosity, layer_ids)
    eta_pad = jnp.pad(viscous, ((1, 1), (1, 1), (0, 0)))

    def apply_op(field_in):
        padded = jnp.pad(field_in, ((0, 0), (2, 2), (2, 2), (0, 0)))

        def slab_apply(j):
            slab_nodes = lax.dynamic_slice_in_dim(padded, j * (2 * ER), 2 * ER + 4, 1)
            slab_visc = lax.dynamic_slice_in_dim(eta_pad, j * ER, ER + 1, 0)
            return stiffness(slab_nodes, slab_visc[:, :NXE + 1])

        pieces = lax.map(slab_apply, jnp.arange(N_RAD, dtype=jnp.int32))
        return jnp.transpose(pieces, (1, 0, 2, 3, 4)).reshape(field_in.shape)

    vectors = [residual]
    for k in range(S):
        vectors.append(apply_op(vectors[-1]) - shifts[k] * vectors[-1])
    new_basis = jnp.stack(vectors[1:], 0)
    stacked = jnp.concatenate([prev_basis, jnp.stack(vectors, 0)], 0).reshape(BASIS, -1)
    gram_matrix = jnp.dot(stacked, stacked.T, precision=lax.Precision.HIGHEST, preferred_element_type=jnp.float32)
    gram_matrix = gram_matrix / (COMP * NRN * NXN * NYN)
    return new_basis, gram_matrix
```

```python
import functools

import jax
import jax.numpy as jnp
from jax import lax
from jax.experimental import pallas as pl
from jax.experimental.pallas import tpu as pltpu
from jax.sharding import PartitionSpec as P

MESH = pl.DeviceIdType.MESH
HIGHEST = lax.Precision.HIGHEST
DEPTH = 2
MASS = (1.0 / 36.0, 1.0 / 12.0, 1.0 / 45.0)
STIFF = (0.0, 1.0, 4.0 / 3.0)
DIRECTIONS = [(dr, dl) for dr in (-1, 1, 0) for dl in (-1, 1, 0) if (dr, dl) != (0, 0)]


def mode_weight(i, j, k):
    return (
        STIFF[i] * MASS[j] * MASS[k]
        + MASS[i] * STIFF[j] * MASS[k]
        + MASS[i] * MASS[j] * STIFF[k]
    )


def to_modes(a, b, c):
    double = b + b
    ends = a + c
    return ends + (double + double), a - c, ends - double


def from_modes(g0, g1, g2):
    ends = g0 + g2
    half = (g0 + g0) - g2
    return ends + g1, half + half, ends - g1


def kernel(
    n_steps, n_prev, n_layers, n_rad, n_lat, dof_count,
    residual, prev_basis, layer_ids, viscosity, shifts,
    new_basis, gram,
    res_v, prev_v, ids_v, pick, pick_t, field, prev_d, wide, parts, pack, side, eta, eta_wide,
    out_v, rows, row_lat, row_rad,
    in_sem, out_sem, send_sem, recv_sem, esend_sem, erecv_sem, gsend_sem, grecv_sem,
):
    rad = lax.axis_index("rad")
    lat = lax.axis_index("lat")
    n_exchange = n_steps // DEPTH
    up = 2 * DEPTH
    down = 2 * DEPTH - 1

    copies = [
        pltpu.make_async_copy(residual, res_v, in_sem.at[0]),
        pltpu.make_async_copy(layer_ids, ids_v, in_sem.at[1]),
        pltpu.make_async_copy(prev_basis, prev_v, in_sem.at[2]),
    ]
    for copy in copies:
        copy.start()

    barrier = pltpu.get_barrier_semaphore()

    def here(dr, dl):
        inside = None
        for value, step, count in ((rad, dr, n_rad), (lat, dl, n_lat)):
            if step:
                test = value < count - 1 if step > 0 else value > 0
                inside = test if inside is None else jnp.logical_and(inside, test)
        return inside

    for d in range(1, n_lat):
        pl.semaphore_signal(
            barrier, inc=1, device_id={"lat": lax.rem(lat + d, n_lat), "rad": rad}, device_id_type=MESH
        )
    for d in range(1, n_rad):
        pl.semaphore_signal(
            barrier, inc=1, device_id={"lat": lat, "rad": lax.rem(rad + d, n_rad)}, device_id_type=MESH
        )
    for dr in (-1, 1):
        for dl in (-1, 1):

            @pl.when(here(dr, dl))
            def _():
                pl.semaphore_signal(
                    barrier, inc=1, device_id={"lat": lat + dl, "rad": rad + dr}, device_id_type=MESH
                )

    rows[...] = jnp.zeros(rows.shape, jnp.float32)
    sub = lax.broadcasted_iota(jnp.int32, (8, 128), 0)
    lane = lax.broadcasted_iota(jnp.int32, (8, 128), 1)
    upper_rows = sub < 4

    row_id = lax.broadcasted_iota(jnp.int32, (256, 256), 0)
    col_id = lax.broadcasted_iota(jnp.int32, (256, 256), 1)
    pick[...] = (row_id == jnp.where(col_id < 128, 2 * col_id, 2 * col_id - 255)).astype(jnp.float32)
    pick_t[...] = (col_id == jnp.where(row_id < 128, 2 * row_id, 2 * row_id - 255)).astype(jnp.float32)

    def split_y(values, store):
        split = jnp.dot(
            values.reshape(192, 256), pick[...], precision=HIGHEST, preferred_element_type=jnp.float32
        )
        for c in range(3):
            block = split[c * 64 : (c + 1) * 64]
            store(0, c, block[:, :128].reshape(8, 8, 128))
            store(1, c, block[:, 128:].reshape(8, 8, 128))

    copies[0].wait()

    def store_field(y, c, value):
        field[0, 4:12, y, c] = value

    split_y(res_v[...], store_field)

    copies[1].wait()
    for a in range(4):
        ids = ids_v[a]
        values = jnp.zeros(ids.shape, jnp.float32)
        for layer in range(n_layers):
            values = jnp.where(ids == layer, viscosity[layer], values)
        eta[1, 2 + a] = jnp.concatenate([values, values], axis=0)

    def pack_sides(e, k):
        for p in range(8):
            for c in range(3):
                even = field[k, 4 + p, 0, c]
                odd = field[k, 4 + p, 1, c]
                pack[e, 0, p, c] = jnp.where(upper_rows, even, pltpu.roll(odd, 4, 0))
                pack[e, 1, p, c] = jnp.where(upper_rows, pltpu.roll(even, 4, 0), odd)

    def halo_copy(e, n):
        dr, dl = DIRECTIONS[n]
        k = e * DEPTH
        source, target, size = {
            1: (8 - up, 4 - up, up), -1: (0, 12, down), 0: (0, 4, 8)
        }[dr]
        if dl == 0:
            src = field.at[k, pl.ds(4 + source, size)]
            dst = field.at[k, pl.ds(target, size)]
        else:
            src = pack.at[e, 0 if dl < 0 else 1, pl.ds(source, size)]
            dst = side.at[e, 1 if dl < 0 else 0, pl.ds(target, size)]
        return pltpu.make_async_remote_copy(
            src_ref=src, dst_ref=dst, send_sem=send_sem.at[e, n], recv_sem=recv_sem.at[e, n],
            device_id={"lat": lat + dl, "rad": rad + dr}, device_id_type=MESH,
        )

    def eta_copy(n):
        dr, dl = DIRECTIONS[n]
        source, target, size = {1: (2, 0, 2), -1: (0, 6, 2), 0: (0, 2, 4)}[dr]
        return pltpu.make_async_remote_copy(
            src_ref=eta.at[1, pl.ds(2 + source, size)],
            dst_ref=eta.at[1 - dl, pl.ds(target, size)],
            send_sem=esend_sem.at[n], recv_sem=erecv_sem.at[n],
            device_id={"lat": lat + dl, "rad": rad + dr}, device_id_type=MESH,
        )

    def each_direction(receive, act):
        for n, (dr, dl) in enumerate(DIRECTIONS):
            test = here(-dr, -dl) if receive else here(dr, dl)

            @pl.when(test)
            def _():
                act(n)

    def widen(p, c, tile, even, odd):
        after = jnp.where(lane < 127, pltpu.roll(even, 127, 1), 0.0)
        for slot, value in enumerate((even, odd, after)):
            wide[p, slot, c, tile * 8 : tile * 8 + 8] = value
            if tile == 0:
                wide[p, slot, c, 16:24] = value

    def widen_own(k, planes):
        for p in planes:
            for c in range(3):
                widen(p, c, 0, field[k, p, 0, c], field[k, p, 1, c])

    def widen_sides(e, planes):
        for p in planes:
            for c in range(3):
                below = side[e, 0, p, c]
                above = side[e, 1, p, c]
                widen(
                    p, c, 1,
                    jnp.where(upper_rows, above, pltpu.roll(below, 4, 0)),
                    jnp.where(upper_rows, pltpu.roll(above, 4, 0), below),
                )

    def dots(n):
        def tile(m, p, y, c):
            return prev_d[m, p, y, c] if m < n_prev else field[m - n_prev, 4 + p, y, c]

        def body(p, sums):
            sums = list(sums)
            for y in range(2):
                for c in range(3):
                    new = tile(n, p, y, c)
                    for m in range(n + 1):
                        other = new if m == n else tile(m, p, y, c)
                        sums[m] = sums[m] + new * other
            return tuple(sums)

        zero = jnp.zeros((8, 128), jnp.float32)
        sums = lax.fori_loop(0, 8, body, (zero,) * (n + 1))
        width = n_prev + n_steps + 1
        for m in range(n + 1):
            total = jnp.sum(sums[m], axis=0, keepdims=True)
            rows[n * width + m : n * width + m + 1] = total
            if m != n:
                rows[m * width + n : m * width + n + 1] = total

    def planes_modes(p, c):
        nodes = [
            [wide[p, slot, c, pl.ds(start, 8, stride=2)] for start in range(3)] for slot in range(3)
        ]
        lines = [to_modes(*nodes[slot]) for slot in range(3)]
        return [to_modes(lines[0][i], lines[1][i], lines[2][i]) for i in range(3)]

    def put_plane(p, c, modes):
        lines = [from_modes(*modes[i]) for i in range(3)]
        for slot in range(3):
            low, mid, high = from_modes(lines[0][slot], lines[1][slot], lines[2][slot])
            parts[p, slot, c, pl.ds(0, 8, stride=2)] = low + pltpu.roll(high, 1, 0)
            parts[p, slot, c, pl.ds(1, 8, stride=2)] = mid

    def apply(first, last, low_plane, high_plane):
        def body(c, nothing):
            below = planes_modes(2 * first, c)
            carried = None
            for a in range(first, last):
                visc = eta_wide[a]
                weight = {}
                for i in range(3):
                    for j in range(i, 3):
                        for l in range(j, 3):
                            if l > 0:
                                weight[i, j, l] = visc * mode_weight(i, j, l)
                middle = planes_modes(2 * a + 1, c)
                above = planes_modes(2 * a + 2, c)
                at_low = [[None] * 3 for _ in range(3)]
                at_mid = [[None] * 3 for _ in range(3)]
                at_high = [[None] * 3 for _ in range(3)]
                for i in range(3):
                    for j in range(3):
                        m = to_modes(below[i][j], middle[i][j], above[i][j])
                        g = [
                            None if i + j + l == 0 else m[l] * weight[tuple(sorted((i, j, l)))]
                            for l in range(3)
                        ]
                        if g[0] is None:
                            twice = g[2] + g[2]
                            out = (g[2] + g[1], -twice, g[2] - g[1])
                        else:
                            out = from_modes(*g)
                        at_low[i][j] = out[0] if carried is None else out[0] + carried[i][j]
                        at_mid[i][j] = out[1]
                        at_high[i][j] = out[2]
                if low_plane <= 2 * a <= high_plane:
                    put_plane(2 * a, c, at_low)
                if low_plane <= 2 * a + 1 <= high_plane:
                    put_plane(2 * a + 1, c, at_mid)
                carried = at_high
                below = above
            return nothing

        lax.fori_loop(0, 3, body, 0)

    keep_rad = jnp.where(rad == n_rad - 1, 0.0, 1.0)
    keep_lat = jnp.where(jnp.logical_and(upper_rows, lat == n_lat - 1), 0.0, 1.0)

    def advance(k, planes, tiles, outer):
        shift = shifts[k]
        for p in planes:
            for c in range(3):
                for tile in tiles:
                    at = slice(tile * 8, tile * 8 + 8)
                    moved = jnp.where(lane > 0, pltpu.roll(parts[p, 2, c, at], 1, 1), 0.0)
                    even = parts[p, 0, c, at] + moved - shift * wide[p, 0, c, at]
                    odd = parts[p, 1, c, at] - shift * wide[p, 1, c, at]
                    if p >= 12:
                        even = even * keep_rad
                        odd = odd * keep_rad
                    if tile == 1:
                        even = even * keep_lat
                        odd = odd * keep_lat
                    if tile == 0 and 4 <= p < 12:
                        field[k + 1, p, 0, c] = even
                        field[k + 1, p, 1, c] = odd
                    if outer:
                        widen(p, c, tile, even, odd)

    def put_out(k):
        lines = []
        for c in range(3):
            even = field[k + 1, 4:12, 0, c].reshape(64, 128)
            odd = field[k + 1, 4:12, 1, c].reshape(64, 128)
            lines.append(jnp.concatenate([even, odd], axis=1))
        merged = jnp.dot(
            jnp.concatenate(lines, axis=0), pick_t[...],
            precision=HIGHEST, preferred_element_type=jnp.float32,
        )
        out_v[k] = merged.reshape(3, 8, 8, 256)
        pltpu.make_async_copy(out_v.at[k], new_basis.at[k], out_sem.at[k]).start()

    def zero_edges():
        blank = jnp.zeros((8, 128), jnp.float32)

        @pl.when(rad == 0)
        def _():
            for e in range(n_exchange):
                field[e * DEPTH, 4 - up : 4] = jnp.broadcast_to(blank, (up, 2, 3, 8, 128))
                side[e, :, 4 - up : 4] = jnp.broadcast_to(blank, (2, up, 3, 8, 128))
            eta[:, 0:2] = jnp.broadcast_to(blank, (3, 2, 8, 128))

        @pl.when(rad == n_rad - 1)
        def _():
            for e in range(n_exchange):
                field[e * DEPTH, 12 : 12 + down] = jnp.broadcast_to(blank, (down, 2, 3, 8, 128))
                side[e, :, 12 : 12 + down] = jnp.broadcast_to(blank, (2, down, 3, 8, 128))
            eta[:, 6:8] = jnp.broadcast_to(blank, (3, 2, 8, 128))

        @pl.when(lat == 0)
        def _():
            for e in range(n_exchange):
                side[e, 0] = jnp.broadcast_to(blank, (16, 3, 8, 128))
            eta[0] = jnp.broadcast_to(blank, (8, 8, 128))

        @pl.when(lat == n_lat - 1)
        def _():
            for e in range(n_exchange):
                side[e, 1] = jnp.broadcast_to(blank, (16, 3, 8, 128))
            eta[2] = jnp.broadcast_to(blank, (8, 8, 128))

    pack_sides(0, 0)
    corners = 0
    for dr in (-1, 1):
        for dl in (-1, 1):
            corners = corners + jnp.where(here(dr, dl), 1, 0)
    pl.semaphore_wait(barrier, n_lat + n_rad - 2 + corners)

    for e in range(n_exchange):
        k = e * DEPTH
        if e == 0:
            each_direction(False, lambda n: eta_copy(n).start())
        each_direction(False, lambda n: halo_copy(e, n).start())
        if e == 0:
            zero_edges()
            widen_own(0, range(4, 12))
            copies[2].wait()
            for m in range(n_prev):

                def store_prev(y, c, value):
                    prev_d[m, :, y, c] = value

                split_y(prev_v[m], store_prev)
            for m in range(n_prev + 1):
                dots(m)
        else:
            for j in range(k - DEPTH + 1, k + 1):
                dots(n_prev + j)
                put_out(j - 1)
        if e == 0:
            each_direction(True, lambda n: eta_copy(n).wait_recv())
            for a in range(8):
                eta_wide[a] = jnp.where(
                    upper_rows, eta[1, a], jnp.where(sub < 6, eta[2, a], eta[0, a])
                )
        each_direction(True, lambda n: halo_copy(e, n).wait_recv())
        low, high = 4 - up, 12 + down
        widen_own(k, list(range(low, 4)) + list(range(12, high)))
        widen_sides(e, range(low, high))
        for step in range(DEPTH):
            left = DEPTH - 1 - step
            apply(1 - left, 6 + left, 4 - 2 * left, 11 + left)
            last = step == DEPTH - 1
            advance(
                k + step, range(4 - 2 * left, 12 + left), (0,) if last else (0, 1),
                not last or e < n_exchange - 1,
            )
        if e < n_exchange - 1:
            pack_sides(e + 1, k + DEPTH)

    for j in range(n_steps - DEPTH + 1, n_steps + 1):
        dots(n_prev + j)
    ones = jnp.ones((8, 128), jnp.float32)
    local = lax.dot_general(
        ones, rows[...], (((1,), (1,)), ((), ())), precision=HIGHEST, preferred_element_type=jnp.float32
    )
    row_lat[lat] = local[0:1]

    def row_copy(stage, d):
        buffer, me, count = (row_lat, lat, n_lat) if stage == 0 else (row_rad, rad, n_rad)
        peer = lax.rem(me + d, count)
        target = {"lat": peer, "rad": rad} if stage == 0 else {"lat": lat, "rad": peer}
        return pltpu.make_async_remote_copy(
            src_ref=buffer.at[me], dst_ref=buffer.at[me],
            send_sem=gsend_sem.at[stage, d], recv_sem=grecv_sem.at[stage, d],
            device_id=target, device_id_type=MESH,
        )

    for d in range(1, n_lat):
        row_copy(0, d).start()
    for j in range(n_steps - DEPTH + 1, n_steps + 1):
        put_out(j - 1)
    for d in range(1, n_lat):
        row_copy(0, d).wait_recv()
    total = row_lat[0]
    for d in range(1, n_lat):
        total = total + row_lat[d]
    row_rad[rad] = total
    for d in range(1, n_rad):
        row_copy(1, d).start()
    for k in range(n_steps):
        pltpu.make_async_copy(out_v.at[k], new_basis.at[k], out_sem.at[k]).wait()
    each_direction(False, lambda n: eta_copy(n).wait_send())
    for e in range(n_exchange):
        each_direction(False, lambda n: halo_copy(e, n).wait_send())
    for d in range(1, n_lat):
        row_copy(0, d).wait_send()
    for d in range(1, n_rad):
        row_copy(1, d).wait_recv()
    total = row_rad[0]
    for d in range(1, n_rad):
        total = total + row_rad[d]
    total = total * (1.0 / dof_count)
    width = n_prev + n_steps + 1
    for i in range(width):
        line = total if i == 0 else pltpu.roll(jnp.broadcast_to(total, (8, 128)), 128 - i * width, 1)[0:1]
        gram[i : i + 1, :] = line[:, :width]
    for d in range(1, n_rad):
        row_copy(1, d).wait_send()


def solution(mesh):
    n_lat = mesh.shape["lat"]
    n_rad = mesh.shape["rad"]

    def on_device(residual, prev_basis, layer_ids, viscosity, shifts):
        n_steps = shifts.shape[0]
        n_prev = prev_basis.shape[0]
        width = n_prev + n_steps + 1
        n_exchange = n_steps // DEPTH
        dof_count = residual.size * n_lat * n_rad
        f32 = jnp.float32
        dma = pltpu.SemaphoreType.DMA
        return pl.pallas_call(
            functools.partial(
                kernel, n_steps, n_prev, viscosity.shape[0], n_rad, n_lat, dof_count
            ),
            out_shape=(
                jax.ShapeDtypeStruct((n_steps,) + residual.shape, f32),
                jax.ShapeDtypeStruct((width, width), f32),
            ),
            in_specs=[pl.BlockSpec(memory_space=pl.ANY)] * 3
            + [pl.BlockSpec(memory_space=pltpu.SMEM)] * 2,
            out_specs=(
                pl.BlockSpec(memory_space=pl.ANY),
                pl.BlockSpec(memory_space=pltpu.VMEM),
            ),
            scratch_shapes=[
                pltpu.VMEM(residual.shape, f32),
                pltpu.VMEM(prev_basis.shape, f32),
                pltpu.VMEM(layer_ids.shape, jnp.int32),
                pltpu.VMEM((256, 256), f32),
                pltpu.VMEM((256, 256), f32),
                pltpu.VMEM((n_steps + 1, 16, 2, 3, 8, 128), f32),
                pltpu.VMEM((n_prev, 8, 2, 3, 8, 128), f32),
                pltpu.VMEM((16, 3, 3, 24, 128), f32),
                pltpu.VMEM((16, 3, 3, 16, 128), f32),
                pltpu.VMEM((n_exchange, 2, 8, 3, 8, 128), f32),
                pltpu.VMEM((n_exchange, 2, 16, 3, 8, 128), f32),
                pltpu.VMEM((3, 8, 8, 128), f32),
                pltpu.VMEM((8, 8, 128), f32),
                pltpu.VMEM((n_steps,) + residual.shape, f32),
                pltpu.VMEM((128, 128), f32),
                pltpu.VMEM((n_lat, 1, 128), f32),
                pltpu.VMEM((n_rad, 1, 128), f32),
                dma((3,)),
                dma((n_steps,)),
                dma((n_exchange, 8)),
                dma((n_exchange, 8)),
                dma((8,)),
                dma((8,)),
                dma((2, max(n_lat, n_rad))),
                dma((2, max(n_lat, n_rad))),
            ],
            compiler_params=pltpu.CompilerParams(collective_id=0, has_side_effects=True),
        )(residual, prev_basis, layer_ids, viscosity, shifts)

    placed = (P(None, "rad", "lat", None), P(None, None, "rad", "lat", None), P("rad", "lat", None), P(), P())
    return jax.shard_map(
        on_device,
        mesh=mesh,
        in_specs=placed,
        out_specs=(P(None, None, "rad", "lat", None), P()),
        check_vma=False,
    )
```

```python
import functools

import jax
import jax.numpy as jnp
from jax import lax
from jax.experimental import pallas as pl
from jax.experimental.pallas import tpu as pltpu
from jax.sharding import PartitionSpec as P

MESH = pl.DeviceIdType.MESH
HIGHEST = lax.Precision.HIGHEST
DEPTH = 2
MASS = (1.0 / 36.0, 1.0 / 12.0, 1.0 / 45.0)
STIFF = (0.0, 1.0, 4.0 / 3.0)
DIRECTIONS = [(dr, dl) for dr in (-1, 1, 0) for dl in (-1, 1, 0) if (dr, dl) != (0, 0)]


def mode_weight(i, j, k):
    return (
        STIFF[i] * MASS[j] * MASS[k]
        + MASS[i] * STIFF[j] * MASS[k]
        + MASS[i] * MASS[j] * STIFF[k]
    )


def to_modes(a, b, c):
    double = b + b
    ends = a + c
    return ends + (double + double), a - c, ends - double


def from_modes(g0, g1, g2):
    ends = g0 + g2
    half = (g0 + g0) - g2
    return ends + g1, half + half, ends - g1


def kernel(
    n_steps, n_prev, n_layers, n_rad, n_lat, dof_count,
    residual, prev_basis, layer_ids, viscosity_in, shifts_in,
    new_basis, gram,
    viscosity, shifts,
    res_v, prev_v, ids_v, pick, pick_t, field, prev_d, wide, parts, pack, side, eta, eta_wide,
    rows, late, row_lat, row_rad,
    known, in_sem, send_sem, recv_sem, esend_sem, erecv_sem, gsend_sem, grecv_sem,
):
    rad = lax.axis_index("rad")
    lat = lax.axis_index("lat")
    n_exchange = n_steps // DEPTH
    up = 2 * DEPTH
    down = 2 * DEPTH - 1

    barrier = pltpu.get_barrier_semaphore()

    def here(dr, dl):
        inside = None
        for value, step, count in ((rad, dr, n_rad), (lat, dl, n_lat)):
            if step:
                test = value < count - 1 if step > 0 else value > 0
                inside = test if inside is None else jnp.logical_and(inside, test)
        return inside

    def around(axis, distance):
        if axis == 0:
            return {"lat": lax.rem(lat + distance + n_lat, n_lat), "rad": rad}
        return {"lat": lat, "rad": lax.rem(rad + distance + n_rad, n_rad)}

    corners = 0
    for axis in range(2):
        for d in (-1, 1):
            pl.semaphore_signal(barrier, inc=1, device_id=around(axis, d), device_id_type=MESH)
    for dr in (-1, 1):
        for dl in (-1, 1):
            corners = corners + jnp.where(here(dr, dl), 1, 0)

            @pl.when(here(dr, dl))
            def _():
                pl.semaphore_signal(
                    barrier, inc=1, device_id={"lat": lat + dl, "rad": rad + dr}, device_id_type=MESH
                )

    def tell(r):
        for axis, count in enumerate((n_lat, n_rad)):
            if 2**r % count:
                for d in (-(2**r), 2**r):
                    pl.semaphore_signal(
                        known.at[axis, r], inc=1, device_id=around(axis, d), device_id_type=MESH
                    )

    def hear(r):
        for axis, count in enumerate((n_lat, n_rad)):
            if 2**r % count:
                pl.semaphore_wait(known.at[axis, r], 2)

    copies = [
        pltpu.make_async_copy(residual, res_v, in_sem.at[0]),
        pltpu.make_async_copy(layer_ids, ids_v, in_sem.at[1]),
        pltpu.make_async_copy(viscosity_in, viscosity, in_sem.at[3]),
        pltpu.make_async_copy(shifts_in, shifts, in_sem.at[4]),
        pltpu.make_async_copy(prev_basis, prev_v, in_sem.at[2]),
    ]
    for copy in copies:
        copy.start()

    rows[...] = jnp.zeros(rows.shape, jnp.float32)
    late[...] = jnp.zeros(late.shape, jnp.float32)
    sub = lax.broadcasted_iota(jnp.int32, (8, 128), 0)
    lane = lax.broadcasted_iota(jnp.int32, (8, 128), 1)
    upper_rows = sub < 4

    row_id = lax.broadcasted_iota(jnp.int32, (256, 256), 0)
    col_id = lax.broadcasted_iota(jnp.int32, (256, 256), 1)
    pick[...] = (row_id == jnp.where(col_id < 128, 2 * col_id, 2 * col_id - 255)).astype(jnp.float32).astype(jnp.bfloat16)
    pick_t[...] = (col_id == jnp.where(row_id < 128, 2 * row_id, 2 * row_id - 255)).astype(jnp.float32).astype(jnp.bfloat16)

    def permute(values, table):
        top = values.astype(jnp.bfloat16)
        rest = values - top.astype(jnp.float32)
        middle = rest.astype(jnp.bfloat16)
        last = (rest - middle.astype(jnp.float32)).astype(jnp.bfloat16)
        moved = jnp.dot(
            jnp.concatenate([top, middle, last], axis=0), table[...], preferred_element_type=jnp.float32
        )
        n = values.shape[0]
        return (moved[:n] + moved[n : 2 * n]) + moved[2 * n :]

    def split_y(values, store):
        split = permute(values.reshape(64, 256), pick)
        store(0, split[:, :128].reshape(8, 8, 128))
        store(1, split[:, 128:].reshape(8, 8, 128))

    def split_residual(c):
        def store(y, value):
            field[0, c, 4:12, y] = value

        split_y(res_v[c], store)

    copies[1].wait()
    copies[2].wait()
    for a in range(4):
        ids = ids_v[a]
        values = jnp.zeros(ids.shape, jnp.float32)
        for layer in range(n_layers):
            values = jnp.where(ids == layer, viscosity[layer], values)
        eta[1, 2 + a] = jnp.concatenate([values, values], axis=0)

    def pack_sides(e, k, c):
        for p in range(8):
            even = field[k, c, 4 + p, 0]
            odd = field[k, c, 4 + p, 1]
            pack[e, c, 0, p] = jnp.where(upper_rows, even, pltpu.roll(odd, 4, 0))
            pack[e, c, 1, p] = jnp.where(upper_rows, pltpu.roll(even, 4, 0), odd)

    def halo_copy(e, c, n):
        dr, dl = DIRECTIONS[n]
        k = e * DEPTH
        source, target, size = {
            1: (8 - up, 4 - up, up), -1: (0, 12, down), 0: (0, 4, 8)
        }[dr]
        if dl == 0:
            src = field.at[k, c, pl.ds(4 + source, size)]
            dst = field.at[k, c, pl.ds(target, size)]
        else:
            src = pack.at[e, c, 0 if dl < 0 else 1, pl.ds(source, size)]
            dst = side.at[e, c, 1 if dl < 0 else 0, pl.ds(target, size)]
        return pltpu.make_async_remote_copy(
            src_ref=src, dst_ref=dst, send_sem=send_sem.at[e, c, n], recv_sem=recv_sem.at[e, c, n],
            device_id={"lat": lat + dl, "rad": rad + dr}, device_id_type=MESH,
        )

    def eta_copy(n):
        dr, dl = DIRECTIONS[n]
        source, target, size = {1: (2, 0, 2), -1: (0, 6, 2), 0: (0, 2, 4)}[dr]
        return pltpu.make_async_remote_copy(
            src_ref=eta.at[1, pl.ds(2 + source, size)],
            dst_ref=eta.at[1 - dl, pl.ds(target, size)],
            send_sem=esend_sem.at[n], recv_sem=erecv_sem.at[n],
            device_id={"lat": lat + dl, "rad": rad + dr}, device_id_type=MESH,
        )

    def each_direction(receive, act):
        for n, (dr, dl) in enumerate(DIRECTIONS):
            test = here(-dr, -dl) if receive else here(dr, dl)

            @pl.when(test)
            def _():
                act(n)

    def put_wide(p, c, tile, values):
        for slot, value in enumerate(values):
            wide[c, p, slot, tile * 8 : tile * 8 + 8] = value
            if tile == 0:
                wide[c, p, slot, 16:24] = value

    def widen(p, c, tile, even, odd):
        put_wide(p, c, tile, (even, odd, jnp.where(lane < 127, pltpu.roll(even, 127, 1), 0.0)))

    def widen_own(k, c, planes):
        for p in planes:
            widen(p, c, 0, field[k, c, p, 0], field[k, c, p, 1])

    def widen_sides(e, c, planes):
        for p in planes:
            below = side[e, c, 0, p]
            above = side[e, c, 1, p]
            widen(
                p, c, 1,
                jnp.where(upper_rows, above, pltpu.roll(below, 4, 0)),
                jnp.where(upper_rows, pltpu.roll(above, 4, 0), below),
            )

    width = n_prev + n_steps + 1

    def dot_sums(n, c, sums):
        def tile(m, p, y):
            return prev_d[m, c, p, y] if m < n_prev else field[m - n_prev, c, 4 + p, y]

        def body(half, sums):
            sums = list(sums)
            for q in range(4):
                for y in range(2):
                    new = tile(n, half * 4 + q, y)
                    for m in range(n + 1):
                        other = new if m == n else tile(m, half * 4 + q, y)
                        sums[m] = sums[m] + new * other
            return tuple(sums)

        return lax.fori_loop(0, 2, body, sums)

    def put_rows(n, sums):
        for m in range(n + 1):
            total = jnp.sum(sums[m], axis=0, keepdims=True)
            rows[n * width + m : n * width + m + 1] = total
            if m != n:
                rows[m * width + n : m * width + n + 1] = total

    def dots(n):
        zero = jnp.zeros((8, 128), jnp.float32)
        put_rows(n, lax.fori_loop(0, 3, lambda c, sums: dot_sums(n, c, sums), (zero,) * (n + 1)))

    def planes_modes(p, c):
        nodes = [
            [wide[c, p, slot, pl.ds(start, 8, stride=2)] for start in range(3)] for slot in range(3)
        ]
        lines = [to_modes(*nodes[slot]) for slot in range(3)]
        return [to_modes(lines[0][i], lines[1][i], lines[2][i]) for i in range(3)]

    def put_plane(p, c, modes):
        lines = [from_modes(*modes[i]) for i in range(3)]
        for slot in range(3):
            low, mid, high = from_modes(lines[0][slot], lines[1][slot], lines[2][slot])
            parts[c, p, slot, pl.ds(0, 8, stride=2)] = low + pltpu.roll(high, 1, 0)
            parts[c, p, slot, pl.ds(1, 8, stride=2)] = mid

    def apply(c, first, last, low_plane, high_plane):
        below = planes_modes(2 * first, c)
        carried = None
        for a in range(first, last):
            visc = eta_wide[a]
            weight = {}
            for i in range(3):
                for j in range(i, 3):
                    for l in range(j, 3):
                        if l > 0:
                            weight[i, j, l] = visc * mode_weight(i, j, l)
            middle = planes_modes(2 * a + 1, c)
            above = planes_modes(2 * a + 2, c)
            at_low = [[None] * 3 for _ in range(3)]
            at_mid = [[None] * 3 for _ in range(3)]
            at_high = [[None] * 3 for _ in range(3)]
            for i in range(3):
                for j in range(3):
                    m = to_modes(below[i][j], middle[i][j], above[i][j])
                    g = [
                        None if i + j + l == 0 else m[l] * weight[tuple(sorted((i, j, l)))]
                        for l in range(3)
                    ]
                    if g[0] is None:
                        twice = g[2] + g[2]
                        out = (g[2] + g[1], -twice, g[2] - g[1])
                    else:
                        out = from_modes(*g)
                    at_low[i][j] = out[0] if carried is None else out[0] + carried[i][j]
                    at_mid[i][j] = out[1]
                    at_high[i][j] = out[2]
            if low_plane <= 2 * a <= high_plane:
                put_plane(2 * a, c, at_low)
            if low_plane <= 2 * a + 1 <= high_plane:
                put_plane(2 * a + 1, c, at_mid)
            carried = at_high
            below = above

    keep_rad = jnp.where(rad == n_rad - 1, 0.0, 1.0)
    keep_lat = jnp.where(jnp.logical_and(upper_rows, lat == n_lat - 1), 0.0, 1.0)

    def advance(k, c, planes, tiles, outer):
        shift = shifts[k]
        for p in planes:
            for tile in tiles:
                at = slice(tile * 8, tile * 8 + 8)
                low = parts[c, p, 0, at]
                high = parts[c, p, 2, at]
                even = low + jnp.where(lane > 0, pltpu.roll(high, 1, 1), 0.0) - shift * wide[c, p, 0, at]
                odd = parts[c, p, 1, at] - shift * wide[c, p, 1, at]
                values = [even, odd]
                if outer:
                    after = jnp.where(lane < 127, pltpu.roll(low, 127, 1) + high, 0.0)
                    values.append(after - shift * wide[c, p, 2, at])
                if p >= 12:
                    values = [value * keep_rad for value in values]
                if tile == 1:
                    values = [value * keep_lat for value in values]
                if tile == 0 and 4 <= p < 12:
                    field[k + 1, c, p, 0] = values[0]
                    field[k + 1, c, p, 1] = values[1]
                if outer:
                    put_wide(p, c, tile, values)

    def put_out(k):
        lines = []
        for c in range(3):
            even = field[k + 1, c, 4:12, 0].reshape(64, 128)
            odd = field[k + 1, c, 4:12, 1].reshape(64, 128)
            lines.append(jnp.concatenate([even, odd], axis=1))
        merged = permute(jnp.concatenate(lines, axis=0), pick_t)
        new_basis[k] = merged.reshape(3, 8, 8, 256)

    def zero_edges():
        def clear(ref):
            ref[...] = jnp.zeros(ref.shape, jnp.float32)

        @pl.when(rad == 0)
        def _():
            for e in range(n_exchange):
                clear(field.at[e * DEPTH, :, 4 - up : 4])
                clear(side.at[e, :, :, 4 - up : 4])
            clear(eta.at[:, 0:2])

        @pl.when(rad == n_rad - 1)
        def _():
            for e in range(n_exchange):
                clear(field.at[e * DEPTH, :, 12 : 12 + down])
                clear(side.at[e, :, :, 12 : 12 + down])
            clear(eta.at[:, 6:8])

        @pl.when(lat == 0)
        def _():
            for e in range(n_exchange):
                clear(side.at[e, :, 0])
            clear(eta.at[0])

        @pl.when(lat == n_lat - 1)
        def _():
            for e in range(n_exchange):
                clear(side.at[e, :, 1])
            clear(eta.at[2])

    def send_halo(e, c):
        each_direction(False, lambda n: halo_copy(e, c, n).start())

    copies[0].wait()
    split_residual(0)
    pack_sides(0, 0, 0)
    pl.semaphore_wait(barrier, 4 + corners)
    each_direction(False, lambda n: eta_copy(n).start())
    send_halo(0, 0)
    for c in range(1, 3):
        split_residual(c)
        pack_sides(0, 0, c)
        send_halo(0, c)
    tell(0)

    zero_edges()
    for c in range(3):
        widen_own(0, c, range(4, 12))
    copies[4].wait()
    copies[3].wait()
    for m in range(n_prev):
        for c in range(3):

            def store_prev(y, value):
                prev_d[m, c, :, y] = value

            split_y(prev_v[m, c], store_prev)
    for m in range(n_prev + 1):
        dots(m)
    hear(0)
    tell(1)
    each_direction(True, lambda n: eta_copy(n).wait_recv())
    for a in range(8):
        eta_wide[a] = jnp.where(upper_rows, eta[1, a], jnp.where(sub < 6, eta[2, a], eta[0, a]))

    low, high = 4 - up, 12 + down
    for e in range(n_exchange):
        k = e * DEPTH
        final = e == n_exchange - 1

        def component(c, nothing):
            each_direction(True, lambda n: halo_copy(e, c, n).wait_recv())
            widen_own(k, c, list(range(low, 4)) + list(range(12, high)))
            widen_sides(e, c, range(low, high))
            for step in range(DEPTH):
                left = DEPTH - 1 - step
                apply(c, 1 - left, 6 + left, 4 - 2 * left, 11 + left)
                last = step == DEPTH - 1
                advance(
                    k + step, c, range(4 - 2 * left, 12 + left), (0,) if last else (0, 1),
                    not (last and final),
                )
            if final:
                for j in range(k + 1, n_steps + 1):
                    n = n_prev + j
                    sums = tuple(late[j - k - 1, m] for m in range(n + 1))
                    for m, value in enumerate(dot_sums(n, c, sums)):
                        late[j - k - 1, m] = value
            else:
                pack_sides(e + 1, k + DEPTH, c)
                send_halo(e + 1, c)
            return nothing

        lax.fori_loop(0, 3, component, 0)
        if not final:
            hear(1)
            tell(2)
            for j in range(k + 1, k + DEPTH + 1):
                dots(n_prev + j)
                put_out(j - 1)

    hear(2)
    for j in range(n_steps - DEPTH + 1, n_steps + 1):
        n = n_prev + j
        put_rows(n, [late[j - (n_steps - DEPTH) - 1, m] for m in range(n + 1)])
    ones = jnp.ones((8, 128), jnp.float32)
    local = lax.dot_general(
        ones, rows[...], (((1,), (1,)), ((), ())), precision=HIGHEST, preferred_element_type=jnp.float32
    )
    row_lat[lat] = local[0:1]

    def row_copy(stage, d):
        buffer, me, count = (row_lat, lat, n_lat) if stage == 0 else (row_rad, rad, n_rad)
        peer = lax.rem(me + d, count)
        target = {"lat": peer, "rad": rad} if stage == 0 else {"lat": lat, "rad": peer}
        return pltpu.make_async_remote_copy(
            src_ref=buffer.at[me], dst_ref=buffer.at[me],
            send_sem=gsend_sem.at[stage, d], recv_sem=grecv_sem.at[stage, d],
            device_id=target, device_id_type=MESH,
        )

    for d in range(1, n_lat):
        row_copy(0, d).start()
    for j in range(n_steps - DEPTH + 1, n_steps + 1):
        put_out(j - 1)
    for d in range(1, n_lat):
        row_copy(0, d).wait_recv()
    total = row_lat[0]
    for d in range(1, n_lat):
        total = total + row_lat[d]
    row_rad[rad] = total
    for d in range(1, n_rad):
        row_copy(1, d).start()
    each_direction(False, lambda n: eta_copy(n).wait_send())
    for e in range(n_exchange):
        for c in range(3):
            each_direction(False, lambda n: halo_copy(e, c, n).wait_send())
    for d in range(1, n_lat):
        row_copy(0, d).wait_send()
    for d in range(1, n_rad):
        row_copy(1, d).wait_recv()
    total = row_rad[0]
    for d in range(1, n_rad):
        total = total + row_rad[d]
    total = total * (1.0 / dof_count)
    for i in range(width):
        line = total if i == 0 else pltpu.roll(jnp.broadcast_to(total, (8, 128)), 128 - i * width, 1)[0:1]
        gram[i : i + 1, :] = line[:, :width]
    for d in range(1, n_rad):
        row_copy(1, d).wait_send()


def solution(mesh):
    n_lat = mesh.shape["lat"]
    n_rad = mesh.shape["rad"]

    def on_device(residual, prev_basis, layer_ids, viscosity, shifts):
        n_steps = shifts.shape[0]
        n_prev = prev_basis.shape[0]
        width = n_prev + n_steps + 1
        n_exchange = n_steps // DEPTH
        dof_count = residual.size * n_lat * n_rad
        f32 = jnp.float32
        dma = pltpu.SemaphoreType.DMA
        return pl.pallas_call(
            functools.partial(
                kernel, n_steps, n_prev, viscosity.shape[0], n_rad, n_lat, dof_count
            ),
            out_shape=(
                jax.ShapeDtypeStruct((n_steps,) + residual.shape, f32),
                jax.ShapeDtypeStruct((width, width), f32),
            ),
            in_specs=[pl.BlockSpec(memory_space=pltpu.HBM)] * 5,
            out_specs=(
                pl.BlockSpec(memory_space=pltpu.VMEM),
                pl.BlockSpec(memory_space=pltpu.VMEM),
            ),
            scratch_shapes=[
                pltpu.SMEM(viscosity.shape, f32),
                pltpu.SMEM(shifts.shape, f32),
                pltpu.VMEM(residual.shape, f32),
                pltpu.VMEM(prev_basis.shape, f32),
                pltpu.VMEM(layer_ids.shape, jnp.int32),
                pltpu.VMEM((256, 256), jnp.bfloat16),
                pltpu.VMEM((256, 256), jnp.bfloat16),
                pltpu.VMEM((n_steps + 1, 3, 16, 2, 8, 128), f32),
                pltpu.VMEM((n_prev, 3, 8, 2, 8, 128), f32),
                pltpu.VMEM((3, 16, 3, 24, 128), f32),
                pltpu.VMEM((3, 16, 3, 16, 128), f32),
                pltpu.VMEM((n_exchange, 3, 2, 8, 8, 128), f32),
                pltpu.VMEM((n_exchange, 3, 2, 16, 8, 128), f32),
                pltpu.VMEM((3, 8, 8, 128), f32),
                pltpu.VMEM((8, 8, 128), f32),
                pltpu.VMEM((128, 128), f32),
                pltpu.VMEM((DEPTH, width, 8, 128), f32),
                pltpu.VMEM((n_lat, 1, 128), f32),
                pltpu.VMEM((n_rad, 1, 128), f32),
                pltpu.SemaphoreType.REGULAR((2, 3)),
                dma((5,)),
                dma((n_exchange, 3, 8)),
                dma((n_exchange, 3, 8)),
                dma((8,)),
                dma((8,)),
                dma((2, max(n_lat, n_rad))),
                dma((2, max(n_lat, n_rad))),
            ],
            compiler_params=pltpu.CompilerParams(collective_id=0, has_side_effects=True, vmem_limit_bytes=24 * 2**20),
        )(*(pltpu.with_memory_space_constraint(x, pltpu.HBM) for x in (residual, prev_basis, layer_ids, viscosity, shifts)))

    placed = (P(None, "rad", "lat", None), P(None, None, "rad", "lat", None), P("rad", "lat", None), P(), P())
    return jax.shard_map(
        on_device,
        mesh=mesh,
        in_specs=placed,
        out_specs=(P(None, None, "rad", "lat", None), P()),
        check_vma=False,
    )
```

```python
import functools

import jax
import jax.numpy as jnp
from jax import lax
from jax.experimental import pallas as pl
from jax.experimental.pallas import tpu as pltpu
from jax.sharding import PartitionSpec as P

MESH = pl.DeviceIdType.MESH
HIGHEST = lax.Precision.HIGHEST
DEPTH = 2
MASS = (1.0 / 36.0, 1.0 / 12.0, 1.0 / 45.0)
STIFF = (0.0, 1.0, 4.0 / 3.0)
DIRECTIONS = [(-1, 0), (1, 0), (-1, -1), (-1, 1), (1, -1), (1, 1), (0, -1), (0, 1)]


def mode_weight(i, j, k):
    return (
        STIFF[i] * MASS[j] * MASS[k]
        + MASS[i] * STIFF[j] * MASS[k]
        + MASS[i] * MASS[j] * STIFF[k]
    )


def to_modes(a, b, c):
    ends = a + c
    return ends + (b + b), a - c, ends - b


def from_modes(g0, g1, g2):
    ends = g0 + g2
    return ends + g1, (g0 + g0) - g2, ends - g1


WEIGHTS = [(i, j, l) for i in range(3) for j in range(i, 3) for l in range(j, 3) if l > 0]


def kernel(
    n_steps, n_prev, n_layers, n_rad, n_lat, dof_count,
    residual, prev_basis, layer_ids, viscosity_in, shifts_in,
    new_basis, gram,
    viscosity, shifts,
    res_v, prev_v, ids_v, pick, pick_t, field, prev_d, wide, parts, pack, side, eta, eta_wide,
    rows, late, row_lat, row_rad,
    known, in_sem, send_sem, recv_sem, esend_sem, erecv_sem, gsend_sem, grecv_sem,
):
    rad = lax.axis_index("rad")
    lat = lax.axis_index("lat")
    n_exchange = n_steps // DEPTH
    up = 2 * DEPTH
    down = 2 * DEPTH - 1

    copies = [
        pltpu.make_async_copy(residual, res_v, in_sem.at[0]),
        pltpu.make_async_copy(layer_ids, ids_v, in_sem.at[1]),
        pltpu.make_async_copy(viscosity_in, viscosity, in_sem.at[3]),
        pltpu.make_async_copy(shifts_in, shifts, in_sem.at[4]),
        pltpu.make_async_copy(prev_basis, prev_v, in_sem.at[2]),
    ]
    for copy in copies:
        copy.start()

    barrier = pltpu.get_barrier_semaphore()

    def here(dr, dl):
        inside = None
        for value, step, count in ((rad, dr, n_rad), (lat, dl, n_lat)):
            if step:
                test = value < count - 1 if step > 0 else value > 0
                inside = test if inside is None else jnp.logical_and(inside, test)
        return inside

    def around(axis, distance):
        if axis == 0:
            return {"lat": lax.rem(lat + distance + n_lat, n_lat), "rad": rad}
        return {"lat": lat, "rad": lax.rem(rad + distance + n_rad, n_rad)}

    corners = 0
    for axis in range(2):
        for d in (-1, 1):
            pl.semaphore_signal(barrier, inc=1, device_id=around(axis, d), device_id_type=MESH)
    for dr in (-1, 1):
        for dl in (-1, 1):
            corners = corners + jnp.where(here(dr, dl), 1, 0)

            @pl.when(here(dr, dl))
            def _():
                pl.semaphore_signal(
                    barrier, inc=1, device_id={"lat": lat + dl, "rad": rad + dr}, device_id_type=MESH
                )

    def tell(r):
        for axis, count in enumerate((n_lat, n_rad)):
            if 2**r % count:
                for d in (-(2**r), 2**r):
                    pl.semaphore_signal(
                        known.at[axis, r], inc=1, device_id=around(axis, d), device_id_type=MESH
                    )

    def hear(r):
        for axis, count in enumerate((n_lat, n_rad)):
            if 2**r % count:
                pl.semaphore_wait(known.at[axis, r], 2)

    rows[...] = jnp.zeros(rows.shape, jnp.float32)
    late[...] = jnp.zeros(late.shape, jnp.float32)
    sub = lax.broadcasted_iota(jnp.int32, (8, 128), 0)
    lane = lax.broadcasted_iota(jnp.int32, (8, 128), 1)
    upper_rows = sub < 4
    double = [jnp.where(sub % 2 == 0, 1.0, 2.0) * 2.0**q for q in range(3)]
    half = [jnp.where(sub % 2 == 0, 1.0, 0.5) * 0.5**q for q in range(3)]
    square = [jnp.where(sub % 2 == 0, 1.0, 4.0) * 4.0**q for q in range(3)]

    row_id = lax.broadcasted_iota(jnp.int32, (256, 256), 0)
    col_id = lax.broadcasted_iota(jnp.int32, (256, 256), 1)
    pick[...] = (row_id == jnp.where(col_id < 128, 2 * col_id, 2 * col_id - 255)).astype(jnp.float32).astype(jnp.bfloat16)
    pick_t[...] = (col_id == jnp.where(row_id < 128, 2 * row_id, 2 * row_id - 255)).astype(jnp.float32).astype(jnp.bfloat16)

    def permute(values, table):
        top = values.astype(jnp.bfloat16)
        rest = values - top.astype(jnp.float32)
        middle = rest.astype(jnp.bfloat16)
        last = (rest - middle.astype(jnp.float32)).astype(jnp.bfloat16)
        moved = jnp.dot(
            jnp.concatenate([top, middle, last], axis=0), table[...], preferred_element_type=jnp.float32
        )
        n = values.shape[0]
        return (moved[:n] + moved[n : 2 * n]) + moved[2 * n :]

    def split_y(values, store):
        split = permute(values.reshape(64, 256), pick)
        store(0, split[:, :128].reshape(8, 8, 128))
        store(1, split[:, 128:].reshape(8, 8, 128))

    def split_residual(c):
        def store(y, value):
            field[0, c, 4:12, y] = value

        split_y(res_v[c], store)

    copies[1].wait()
    copies[2].wait()
    layers = []
    for a in range(4):
        ids = ids_v[a]
        values = jnp.zeros(ids.shape, jnp.float32)
        for layer in range(n_layers):
            values = jnp.where(ids == layer, viscosity[layer], values)
        layers.append(values)

    for h in range(2):
        eta[1, 1 + h] = jnp.concatenate(layers[2 * h : 2 * h + 2], axis=0)

    def pack_sides(e, k, c):
        for p in range(8):
            even = field[k, c, 4 + p, 0]
            odd = field[k, c, 4 + p, 1]
            pack[e, c, 0, p] = jnp.where(upper_rows, even, pltpu.roll(odd, 4, 0))
            pack[e, c, 1, p] = jnp.where(upper_rows, pltpu.roll(even, 4, 0), odd)

    def halo_copy(e, c, n):
        dr, dl = DIRECTIONS[n]
        k = e * DEPTH
        source, target, size = {
            1: (8 - up, 4 - up, up), -1: (0, 12, down), 0: (0, 4, 8)
        }[dr]
        if dl == 0:
            src = field.at[k, c, pl.ds(4 + source, size)]
            dst = field.at[k, c, pl.ds(target, size)]
        else:
            src = pack.at[e, c, 0 if dl < 0 else 1, pl.ds(source, size)]
            dst = side.at[e, c, 1 if dl < 0 else 0, pl.ds(target, size)]
        return pltpu.make_async_remote_copy(
            src_ref=src, dst_ref=dst, send_sem=send_sem.at[e, c, n], recv_sem=recv_sem.at[e, c, n],
            device_id={"lat": lat + dl, "rad": rad + dr}, device_id_type=MESH,
        )

    def eta_copy(n):
        dr, dl = DIRECTIONS[n]
        source, target, size = {1: (1, 0, 1), -1: (0, 3, 1), 0: (0, 1, 2)}[dr]
        return pltpu.make_async_remote_copy(
            src_ref=eta.at[1, pl.ds(1 + source, size)],
            dst_ref=eta.at[1 - dl, pl.ds(target, size)],
            send_sem=esend_sem.at[n], recv_sem=erecv_sem.at[n],
            device_id={"lat": lat + dl, "rad": rad + dr}, device_id_type=MESH,
        )

    def each_direction(receive, act, which=range(8)):
        for n, (dr, dl) in enumerate(DIRECTIONS):
            if n not in which:
                continue
            test = here(-dr, -dl) if receive else here(dr, dl)

            @pl.when(test)
            def _():
                act(n)

    def put_wide(p, c, tile, values):
        for slot, value in enumerate(values):
            wide[c, p, slot, tile * 8 : tile * 8 + 8] = value
            if tile == 0:
                wide[c, p, slot, 16:24] = value

    def widen(p, c, tile, even, odd):
        even = even * double[p % 2]
        odd = odd * double[p % 2 + 1]
        put_wide(p, c, tile, (even, odd, jnp.where(lane < 127, pltpu.roll(even, 127, 1), 0.0)))

    def widen_own(k, c, planes):
        for p in planes:
            widen(p, c, 0, field[k, c, p, 0], field[k, c, p, 1])

    def widen_sides(e, c, planes):
        for p in planes:
            below = side[e, c, 0, p]
            above = side[e, c, 1, p]
            widen(
                p, c, 1,
                jnp.where(upper_rows, above, pltpu.roll(below, 4, 0)),
                jnp.where(upper_rows, pltpu.roll(above, 4, 0), below),
            )

    width = n_prev + n_steps + 1

    def dot_sums(n, c, sums):
        def tile(m, p, y):
            return prev_d[m, c, p, y] if m < n_prev else field[m - n_prev, c, 4 + p, y]

        def body(half, sums):
            sums = list(sums)
            for q in range(4):
                for y in range(2):
                    new = tile(n, half * 4 + q, y)
                    for m in range(n + 1):
                        other = new if m == n else tile(m, half * 4 + q, y)
                        sums[m] = sums[m] + new * other
            return tuple(sums)

        return lax.fori_loop(0, 2, body, sums)

    def put_rows(n, sums):
        for m in range(n + 1):
            total = jnp.sum(sums[m], axis=0, keepdims=True)
            rows[n * width + m : n * width + m + 1] = total
            if m != n:
                rows[m * width + n : m * width + n + 1] = total

    def dots(n):
        zero = jnp.zeros((8, 128), jnp.float32)
        put_rows(n, lax.fori_loop(0, 3, lambda c, sums: dot_sums(n, c, sums), (zero,) * (n + 1)))

    def planes_modes(p, c):
        nodes = [
            [wide[c, p, slot, pl.ds(start, 8, stride=2)] for start in range(3)] for slot in range(3)
        ]
        lines = [to_modes(*nodes[slot]) for slot in range(3)]
        return [to_modes(lines[0][i], lines[1][i], lines[2][i]) for i in range(3)]

    def put_plane(p, c, modes):
        lines = [from_modes(*modes[i]) for i in range(3)]
        for slot in range(3):
            low, mid, high = from_modes(lines[0][slot], lines[1][slot], lines[2][slot])
            parts[c, p, slot, pl.ds(0, 8, stride=2)] = low + pltpu.roll(high, 1, 0)
            parts[c, p, slot, pl.ds(1, 8, stride=2)] = mid

    def apply(c, first, last, low_plane, high_plane):
        below = planes_modes(2 * first, c)
        carried = None
        for a in range(first, last):
            middle = planes_modes(2 * a + 1, c)
            above = planes_modes(2 * a + 2, c)
            at_low = [[None] * 3 for _ in range(3)]
            at_mid = [[None] * 3 for _ in range(3)]
            at_high = [[None] * 3 for _ in range(3)]
            for i in range(3):
                for j in range(3):
                    m = to_modes(below[i][j], middle[i][j], above[i][j])
                    g = [
                        None if i + j + l == 0 else m[l] * eta_wide[a, WEIGHTS.index(tuple(sorted((i, j, l))))]
                        for l in range(3)
                    ]
                    if g[0] is None:
                        out = (g[2] + g[1], -g[2], g[2] - g[1])
                    else:
                        out = from_modes(*g)
                    at_low[i][j] = out[0] if carried is None else out[0] + carried[i][j]
                    at_mid[i][j] = out[1]
                    at_high[i][j] = out[2]
            if low_plane <= 2 * a <= high_plane:
                put_plane(2 * a, c, at_low)
            if low_plane <= 2 * a + 1 <= high_plane:
                put_plane(2 * a + 1, c, at_mid)
            carried = at_high
            below = above

    keep_rad = jnp.where(rad == n_rad - 1, 0.0, 1.0)
    keep_lat = jnp.where(jnp.logical_and(upper_rows, lat == n_lat - 1), 0.0, 1.0)

    def advance(k, c, planes, tiles, outer):
        shift = shifts[k]
        for p in planes:
            for tile in tiles:
                at = slice(tile * 8, tile * 8 + 8)
                low = parts[c, p, 0, at]
                high = parts[c, p, 2, at]
                moved = jnp.where(lane > 0, pltpu.roll(high, 1, 1), 0.0)
                even = square[p % 2] * (low + moved) - shift * wide[c, p, 0, at]
                odd = square[p % 2 + 1] * parts[c, p, 1, at] - shift * wide[c, p, 1, at]
                values = [even, odd]
                if outer:
                    after = jnp.where(lane < 127, pltpu.roll(low, 127, 1) + high, 0.0)
                    values.append(square[p % 2] * after - shift * wide[c, p, 2, at])
                if p >= 12:
                    values = [value * keep_rad for value in values]
                if tile == 1:
                    values = [value * keep_lat for value in values]
                if tile == 0 and 4 <= p < 12:
                    field[k + 1, c, p, 0] = values[0] * half[p % 2]
                    field[k + 1, c, p, 1] = values[1] * half[p % 2 + 1]
                if outer:
                    put_wide(p, c, tile, values)

    def put_out(k):
        lines = []
        for c in range(3):
            even = field[k + 1, c, 4:12, 0].reshape(64, 128)
            odd = field[k + 1, c, 4:12, 1].reshape(64, 128)
            lines.append(jnp.concatenate([even, odd], axis=1))
        merged = permute(jnp.concatenate(lines, axis=0), pick_t)
        new_basis[k] = merged.reshape(3, 8, 8, 256)

    def zero_edges():
        def clear(ref):
            ref[...] = jnp.zeros(ref.shape, jnp.float32)

        @pl.when(rad == 0)
        def _():
            for e in range(n_exchange):
                clear(field.at[e * DEPTH, :, 4 - up : 4])
                clear(side.at[e, :, :, 4 - up : 4])
            clear(eta.at[:, 0:1])

        @pl.when(rad == n_rad - 1)
        def _():
            for e in range(n_exchange):
                clear(field.at[e * DEPTH, :, 12 : 12 + down])
                clear(side.at[e, :, :, 12 : 12 + down])
            clear(eta.at[:, 3:4])

        @pl.when(lat == 0)
        def _():
            for e in range(n_exchange):
                clear(side.at[e, :, 0])
            clear(eta.at[0])

        @pl.when(lat == n_lat - 1)
        def _():
            for e in range(n_exchange):
                clear(side.at[e, :, 1])
            clear(eta.at[2])

    def send_halo(e, c, which=range(8)):
        each_direction(False, lambda n: halo_copy(e, c, n).start(), which)

    copies[0].wait()
    split_residual(0)
    pack_sides(0, 0, 0)
    pl.semaphore_wait(barrier, 4 + corners)
    each_direction(False, lambda n: eta_copy(n).start())
    send_halo(0, 0)
    for c in range(1, 3):
        split_residual(c)
        pack_sides(0, 0, c)
        send_halo(0, c)
    tell(0)

    zero_edges()
    for c in range(3):
        widen_own(0, c, range(4, 12))
    copies[4].wait()
    copies[3].wait()
    for m in range(n_prev):
        for c in range(3):

            def store_prev(y, value):
                prev_d[m, c, :, y] = value

            split_y(prev_v[m, c], store_prev)
    for m in range(n_prev + 1):
        dots(m)
    hear(0)
    tell(1)
    each_direction(True, lambda n: eta_copy(n).wait_recv())
    for h in range(4):
        own = eta[1, h]
        beside = jnp.where(sub % 4 < 2, eta[2, h], eta[0, h])
        for half_row, visc in enumerate((
            jnp.where(upper_rows, own, pltpu.roll(beside, 4, 0)),
            jnp.where(upper_rows, pltpu.roll(own, 4, 0), beside),
        )):
            for q, modes in enumerate(WEIGHTS):
                eta_wide[2 * h + half_row, q] = visc * mode_weight(*modes)

    low, high = 4 - up, 12 + down
    for e in range(n_exchange):
        k = e * DEPTH
        final = e == n_exchange - 1

        def component(c, nothing):
            each_direction(True, lambda n: halo_copy(e, c, n).wait_recv())
            widen_own(k, c, list(range(low, 4)) + list(range(12, high)))
            widen_sides(e, c, range(low, high))
            for step in range(DEPTH):
                left = DEPTH - 1 - step
                apply(c, 1 - left, 6 + left, 4 - 2 * left, 11 + left)
                last = step == DEPTH - 1
                advance(
                    k + step, c, range(4 - 2 * left, 12 + left), (0,) if last else (0, 1),
                    not (last and final),
                )
            if final:
                for j in range(k + 1, n_steps + 1):
                    n = n_prev + j
                    sums = tuple(late[j - k - 1, m] for m in range(n + 1))
                    for m, value in enumerate(dot_sums(n, c, sums)):
                        late[j - k - 1, m] = value
            else:
                send_halo(e + 1, c, range(2))
                pack_sides(e + 1, k + DEPTH, c)
                send_halo(e + 1, c, range(2, 8))
            return nothing

        lax.fori_loop(0, 3, component, 0)
        if not final:
            hear(1)
            tell(2)
            for j in range(k + 1, k + DEPTH + 1):
                dots(n_prev + j)
                put_out(j - 1)

    hear(2)
    for j in range(n_steps - DEPTH + 1, n_steps + 1):
        n = n_prev + j
        put_rows(n, [late[j - (n_steps - DEPTH) - 1, m] for m in range(n + 1)])
    ones = jnp.ones((8, 128), jnp.float32)
    local = lax.dot_general(
        ones, rows[...], (((1,), (1,)), ((), ())), precision=HIGHEST, preferred_element_type=jnp.float32
    )
    row_lat[lat] = local[0:1]

    def row_copy(stage, d):
        buffer, me, count = (row_lat, lat, n_lat) if stage == 0 else (row_rad, rad, n_rad)
        peer = lax.rem(me + d, count)
        target = {"lat": peer, "rad": rad} if stage == 0 else {"lat": lat, "rad": peer}
        return pltpu.make_async_remote_copy(
            src_ref=buffer.at[me], dst_ref=buffer.at[me],
            send_sem=gsend_sem.at[stage, d], recv_sem=grecv_sem.at[stage, d],
            device_id=target, device_id_type=MESH,
        )

    for d in range(1, n_lat):
        row_copy(0, d).start()
    for j in range(n_steps - DEPTH + 1, n_steps + 1):
        put_out(j - 1)
    for d in range(1, n_lat):
        row_copy(0, d).wait_recv()
    total = row_lat[0]
    for d in range(1, n_lat):
        total = total + row_lat[d]
    row_rad[rad] = total
    for d in range(1, n_rad):
        row_copy(1, d).start()
    each_direction(False, lambda n: eta_copy(n).wait_send())
    for e in range(n_exchange):
        for c in range(3):
            each_direction(False, lambda n: halo_copy(e, c, n).wait_send())
    for d in range(1, n_lat):
        row_copy(0, d).wait_send()
    for d in range(1, n_rad):
        row_copy(1, d).wait_recv()
    total = row_rad[0]
    for d in range(1, n_rad):
        total = total + row_rad[d]
    total = total * (1.0 / dof_count)
    for i in range(width):
        line = total if i == 0 else pltpu.roll(jnp.broadcast_to(total, (8, 128)), 128 - i * width, 1)[0:1]
        gram[i : i + 1, :] = line[:, :width]
    for d in range(1, n_rad):
        row_copy(1, d).wait_send()


def leave(vectors, sums, new_basis, gram, sems):
    copies = [
        pltpu.make_async_copy(vectors, new_basis, sems.at[0]),
        pltpu.make_async_copy(sums, gram, sems.at[1]),
    ]
    for copy in copies:
        copy.start()
    for copy in copies:
        copy.wait()


def solution(mesh):
    n_lat = mesh.shape["lat"]
    n_rad = mesh.shape["rad"]

    def on_device(residual, prev_basis, layer_ids, viscosity, shifts):
        n_steps = shifts.shape[0]
        n_prev = prev_basis.shape[0]
        width = n_prev + n_steps + 1
        n_exchange = n_steps // DEPTH
        dof_count = residual.size * n_lat * n_rad
        f32 = jnp.float32
        dma = pltpu.SemaphoreType.DMA
        vectors, sums = pl.pallas_call(
            functools.partial(
                kernel, n_steps, n_prev, viscosity.shape[0], n_rad, n_lat, dof_count
            ),
            out_shape=(
                jax.ShapeDtypeStruct((n_steps,) + residual.shape, f32),
                jax.ShapeDtypeStruct((width, width), f32),
            ),
            in_specs=[pl.BlockSpec(memory_space=pltpu.HBM)] * 5,
            out_specs=(
                pl.BlockSpec(memory_space=pltpu.VMEM),
                pl.BlockSpec(memory_space=pltpu.VMEM),
            ),
            scratch_shapes=[
                pltpu.SMEM(viscosity.shape, f32),
                pltpu.SMEM(shifts.shape, f32),
                pltpu.VMEM(residual.shape, f32),
                pltpu.VMEM(prev_basis.shape, f32),
                pltpu.VMEM(layer_ids.shape, jnp.int32),
                pltpu.VMEM((256, 256), jnp.bfloat16),
                pltpu.VMEM((256, 256), jnp.bfloat16),
                pltpu.VMEM((n_steps + 1, 3, 16, 2, 8, 128), f32),
                pltpu.VMEM((n_prev, 3, 8, 2, 8, 128), f32),
                pltpu.VMEM((3, 16, 3, 24, 128), f32),
                pltpu.VMEM((3, 16, 3, 16, 128), f32),
                pltpu.VMEM((n_exchange, 3, 2, 8, 8, 128), f32),
                pltpu.VMEM((n_exchange, 3, 2, 16, 8, 128), f32),
                pltpu.VMEM((3, 4, 8, 128), f32),
                pltpu.VMEM((8, len(WEIGHTS), 8, 128), f32),
                pltpu.VMEM((128, 128), f32),
                pltpu.VMEM((DEPTH, width, 8, 128), f32),
                pltpu.VMEM((n_lat, 1, 128), f32),
                pltpu.VMEM((n_rad, 1, 128), f32),
                pltpu.SemaphoreType.REGULAR((2, 3)),
                dma((5,)),
                dma((n_exchange, 3, 8)),
                dma((n_exchange, 3, 8)),
                dma((8,)),
                dma((8,)),
                dma((2, max(n_lat, n_rad))),
                dma((2, max(n_lat, n_rad))),
            ],
            compiler_params=pltpu.CompilerParams(collective_id=0, has_side_effects=True, vmem_limit_bytes=24 * 2**20),
        )(*(pltpu.with_memory_space_constraint(x, pltpu.HBM) for x in (residual, prev_basis, layer_ids, viscosity, shifts)))

        return pl.pallas_call(
            leave,
            out_shape=(
                jax.ShapeDtypeStruct(vectors.shape, f32),
                jax.ShapeDtypeStruct(sums.shape, f32),
            ),
            in_specs=[pl.BlockSpec(memory_space=pltpu.VMEM)] * 2,
            out_specs=(pl.BlockSpec(memory_space=pltpu.HBM), pl.BlockSpec(memory_space=pltpu.HBM)),
            scratch_shapes=[dma((2,))],
            compiler_params=pltpu.CompilerParams(vmem_limit_bytes=2**20),
        )(vectors, sums)

    placed = (P(None, "rad", "lat", None), P(None, None, "rad", "lat", None), P("rad", "lat", None), P(), P())
    return jax.shard_map(
        on_device,
        mesh=mesh,
        in_specs=placed,
        out_specs=(P(None, None, "rad", "lat", None), P()),
        check_vma=False,
    )
```

```python
import functools

import jax
import jax.numpy as jnp
from jax import lax
from jax.experimental import pallas as pl
from jax.experimental.pallas import tpu as pltpu
from jax.sharding import PartitionSpec as P

MESH = pl.DeviceIdType.MESH
HIGHEST = lax.Precision.HIGHEST
DEPTH = 2
MASS = (1.0 / 36.0, 1.0 / 12.0, 1.0 / 45.0)
STIFF = (0.0, 1.0, 4.0 / 3.0)
DIRECTIONS = [(-1, 0), (1, 0), (-1, -1), (-1, 1), (1, -1), (1, 1), (0, -1), (0, 1)]


def mode_weight(i, j, k):
    return (
        STIFF[i] * MASS[j] * MASS[k]
        + MASS[i] * STIFF[j] * MASS[k]
        + MASS[i] * MASS[j] * STIFF[k]
    )


def to_modes(a, b, c):
    ends = a + c
    return ends + (b + b), a - c, ends - b


def from_modes(g0, g1, g2):
    ends = g0 + g2
    return ends + g1, (g0 + g0) - g2, ends - g1


WEIGHTS = [(i, j, l) for i in range(3) for j in range(i, 3) for l in range(j, 3) if l > 0]


def kernel(
    n_steps, n_prev, n_layers, n_rad, n_lat,
    residual, prev_basis, layer_ids, viscosity_in, shifts_in,
    new_basis, gram,
    viscosity, shifts,
    res_v, prev_v, ids_v, pick, pick_t, field, prev_d, wide, parts, pack, side, eta, eta_wide,
    rows, late, row_lat, row_rad,
    known, in_sem, send_sem, recv_sem, esend_sem, erecv_sem, gsend_sem, grecv_sem,
):
    rad = lax.axis_index("rad")
    lat = lax.axis_index("lat")
    n_exchange = n_steps // DEPTH
    up = 2 * DEPTH
    down = 2 * DEPTH - 1

    copies = [
        pltpu.make_async_copy(residual, res_v, in_sem.at[0]),
        pltpu.make_async_copy(layer_ids, ids_v, in_sem.at[1]),
        pltpu.make_async_copy(viscosity_in, viscosity, in_sem.at[3]),
        pltpu.make_async_copy(shifts_in, shifts, in_sem.at[4]),
        pltpu.make_async_copy(prev_basis, prev_v, in_sem.at[2]),
    ]
    for copy in copies:
        copy.start()

    barrier = pltpu.get_barrier_semaphore()

    def here(dr, dl):
        inside = None
        for value, step, count in ((rad, dr, n_rad), (lat, dl, n_lat)):
            if step:
                test = value < count - 1 if step > 0 else value > 0
                inside = test if inside is None else jnp.logical_and(inside, test)
        return inside

    def around(axis, distance):
        if axis == 0:
            return {"lat": lax.rem(lat + distance + n_lat, n_lat), "rad": rad}
        return {"lat": lat, "rad": lax.rem(rad + distance + n_rad, n_rad)}

    corners = 0
    for axis in range(2):
        for d in (-1, 1):
            pl.semaphore_signal(barrier, inc=1, device_id=around(axis, d), device_id_type=MESH)
    for dr in (-1, 1):
        for dl in (-1, 1):
            corners = corners + jnp.where(here(dr, dl), 1, 0)

            @pl.when(here(dr, dl))
            def _():
                pl.semaphore_signal(
                    barrier, inc=1, device_id={"lat": lat + dl, "rad": rad + dr}, device_id_type=MESH
                )

    def tell(r):
        for axis, count in enumerate((n_lat, n_rad)):
            if 2**r % count:
                for d in (-(2**r), 2**r):
                    pl.semaphore_signal(
                        known.at[axis, r], inc=1, device_id=around(axis, d), device_id_type=MESH
                    )

    def hear(r):
        for axis, count in enumerate((n_lat, n_rad)):
            if 2**r % count:
                pl.semaphore_wait(known.at[axis, r], 2)

    sub = lax.broadcasted_iota(jnp.int32, (8, 128), 0)
    lane = lax.broadcasted_iota(jnp.int32, (8, 128), 1)
    upper_rows = sub < 4
    double = [jnp.where(sub % 2 == 0, 1.0, 2.0) * 2.0**q for q in range(3)]
    half = [jnp.where(sub % 2 == 0, 1.0, 0.5) * 0.5**q for q in range(3)]
    square = [jnp.where(sub % 2 == 0, 1.0, 4.0) * 4.0**q for q in range(3)]

    row_id = lax.broadcasted_iota(jnp.int32, (256, 256), 0)
    col_id = lax.broadcasted_iota(jnp.int32, (256, 256), 1)
    pick[...] = (row_id == jnp.where(col_id < 128, 2 * col_id, 2 * col_id - 255)).astype(jnp.float32).astype(jnp.bfloat16)

    def permute(values, table):
        top = values.astype(jnp.bfloat16)
        rest = values - top.astype(jnp.float32)
        middle = rest.astype(jnp.bfloat16)
        last = (rest - middle.astype(jnp.float32)).astype(jnp.bfloat16)
        moved = jnp.dot(
            jnp.concatenate([top, middle, last], axis=0), table[...], preferred_element_type=jnp.float32
        )
        n = values.shape[0]
        return (moved[:n] + moved[n : 2 * n]) + moved[2 * n :]

    def split_y(values, store):
        split = permute(values.reshape(64, 256), pick)
        store(0, split[:, :128].reshape(8, 8, 128))
        store(1, split[:, 128:].reshape(8, 8, 128))

    def split_residual(c):
        def store(y, value):
            field[0, c, 4:12, y] = value

        split_y(res_v[c], store)

    copies[1].wait()
    copies[2].wait()
    layers = []
    for a in range(4):
        ids = ids_v[a]
        values = jnp.zeros(ids.shape, jnp.float32)
        for layer in range(n_layers):
            values = jnp.where(ids == layer, viscosity[layer], values)
        layers.append(values)

    for h in range(2):
        eta[1, 1 + h] = jnp.concatenate(layers[2 * h : 2 * h + 2], axis=0)

    def pack_sides(e, k, c):
        for p in range(8):
            even = field[k, c, 4 + p, 0]
            odd = field[k, c, 4 + p, 1]
            pack[e, c, 0, p] = jnp.where(upper_rows, even, pltpu.roll(odd, 4, 0))
            pack[e, c, 1, p] = jnp.where(upper_rows, pltpu.roll(even, 4, 0), odd)

    def halo_copy(e, c, n):
        dr, dl = DIRECTIONS[n]
        k = e * DEPTH
        source, target, size = {
            1: (8 - up, 4 - up, up), -1: (0, 12, down), 0: (0, 4, 8)
        }[dr]
        if dl == 0:
            src = field.at[k, c, pl.ds(4 + source, size)]
            dst = field.at[k, c, pl.ds(target, size)]
        else:
            src = pack.at[e, c, 0 if dl < 0 else 1, pl.ds(source, size)]
            dst = side.at[e, c, 1 if dl < 0 else 0, pl.ds(target, size)]
        return pltpu.make_async_remote_copy(
            src_ref=src, dst_ref=dst, send_sem=send_sem.at[e, c, n], recv_sem=recv_sem.at[e, c, n],
            device_id={"lat": lat + dl, "rad": rad + dr}, device_id_type=MESH,
        )

    def eta_copy(n):
        dr, dl = DIRECTIONS[n]
        source, target, size = {1: (1, 0, 1), -1: (0, 3, 1), 0: (0, 1, 2)}[dr]
        return pltpu.make_async_remote_copy(
            src_ref=eta.at[1, pl.ds(1 + source, size)],
            dst_ref=eta.at[1 - dl, pl.ds(target, size)],
            send_sem=esend_sem.at[n], recv_sem=erecv_sem.at[n],
            device_id={"lat": lat + dl, "rad": rad + dr}, device_id_type=MESH,
        )

    def each_direction(receive, act, which=range(8)):
        for n, (dr, dl) in enumerate(DIRECTIONS):
            if n not in which:
                continue
            test = here(-dr, -dl) if receive else here(dr, dl)

            @pl.when(test)
            def _():
                act(n)

    def put_wide(p, c, tile, values):
        for slot, value in enumerate(values):
            wide[c, p, slot, tile * 8 : tile * 8 + 8] = value
            if tile == 0:
                wide[c, p, slot, 16:24] = value

    def widen(p, c, tile, even, odd):
        even = even * double[p % 2]
        odd = odd * double[p % 2 + 1]
        put_wide(p, c, tile, (even, odd, jnp.where(lane < 127, pltpu.roll(even, 127, 1), 0.0)))

    def widen_own(k, c, planes):
        for p in planes:
            widen(p, c, 0, field[k, c, p, 0], field[k, c, p, 1])

    def widen_sides(e, c, planes):
        for p in planes:
            below = side[e, c, 0, p]
            above = side[e, c, 1, p]
            widen(
                p, c, 1,
                jnp.where(upper_rows, above, pltpu.roll(below, 4, 0)),
                jnp.where(upper_rows, pltpu.roll(above, 4, 0), below),
            )

    width = n_prev + n_steps + 1

    def dot_sums(n, c, sums):
        def tile(m, p, y):
            return prev_d[m, c, p, y] if m < n_prev else field[m - n_prev, c, 4 + p, y]

        def body(half, sums):
            sums = list(sums)
            for q in range(4):
                for y in range(2):
                    new = tile(n, half * 4 + q, y)
                    for m in range(n + 1):
                        other = new if m == n else tile(m, half * 4 + q, y)
                        sums[m] = sums[m] + new * other
            return tuple(sums)

        return lax.fori_loop(0, 2, body, sums)

    def put_rows(n, sums):
        for m in range(n + 1):
            total = jnp.sum(sums[m], axis=0, keepdims=True)
            rows[n * width + m : n * width + m + 1] = total
            if m != n:
                rows[m * width + n : m * width + n + 1] = total

    def dots(n):
        zero = jnp.zeros((8, 128), jnp.float32)
        put_rows(n, lax.fori_loop(0, 3, lambda c, sums: dot_sums(n, c, sums), (zero,) * (n + 1)))

    def planes_modes(p, c):
        nodes = [
            [wide[c, p, slot, pl.ds(start, 8, stride=2)] for start in range(3)] for slot in range(3)
        ]
        lines = [to_modes(*nodes[slot]) for slot in range(3)]
        return [to_modes(lines[0][i], lines[1][i], lines[2][i]) for i in range(3)]

    def put_plane(p, c, modes):
        lines = [from_modes(*modes[i]) for i in range(3)]
        for slot in range(3):
            low, mid, high = from_modes(lines[0][slot], lines[1][slot], lines[2][slot])
            parts[c, p, slot, pl.ds(0, 8, stride=2)] = low + pltpu.roll(high, 1, 0)
            parts[c, p, slot, pl.ds(1, 8, stride=2)] = mid

    def apply(c, first, last, low_plane, high_plane):
        below = planes_modes(2 * first, c)
        carried = None
        for a in range(first, last):
            middle = planes_modes(2 * a + 1, c)
            above = planes_modes(2 * a + 2, c)
            at_low = [[None] * 3 for _ in range(3)]
            at_mid = [[None] * 3 for _ in range(3)]
            at_high = [[None] * 3 for _ in range(3)]
            for i in range(3):
                for j in range(3):
                    m = to_modes(below[i][j], middle[i][j], above[i][j])
                    g = [
                        None if i + j + l == 0 else m[l] * eta_wide[a, WEIGHTS.index(tuple(sorted((i, j, l))))]
                        for l in range(3)
                    ]
                    if g[0] is None:
                        out = (g[2] + g[1], -g[2], g[2] - g[1])
                    else:
                        out = from_modes(*g)
                    at_low[i][j] = out[0] if carried is None else out[0] + carried[i][j]
                    at_mid[i][j] = out[1]
                    at_high[i][j] = out[2]
            if low_plane <= 2 * a <= high_plane:
                put_plane(2 * a, c, at_low)
            if low_plane <= 2 * a + 1 <= high_plane:
                put_plane(2 * a + 1, c, at_mid)
            carried = at_high
            below = above

    keep_rad = jnp.where(rad == n_rad - 1, 0.0, 1.0)
    keep_lat = jnp.where(jnp.logical_and(upper_rows, lat == n_lat - 1), 0.0, 1.0)

    def advance(k, c, planes, tiles, outer):
        shift = shifts[k]
        for p in planes:
            for tile in tiles:
                at = slice(tile * 8, tile * 8 + 8)
                low = parts[c, p, 0, at]
                high = parts[c, p, 2, at]
                moved = jnp.where(lane > 0, pltpu.roll(high, 1, 1), 0.0)
                even = square[p % 2] * (low + moved) - shift * wide[c, p, 0, at]
                odd = square[p % 2 + 1] * parts[c, p, 1, at] - shift * wide[c, p, 1, at]
                values = [even, odd]
                if outer:
                    after = jnp.where(lane < 127, pltpu.roll(low, 127, 1) + high, 0.0)
                    values.append(square[p % 2] * after - shift * wide[c, p, 2, at])
                if p >= 12:
                    values = [value * keep_rad for value in values]
                if tile == 1:
                    values = [value * keep_lat for value in values]
                if tile == 0 and 4 <= p < 12:
                    field[k + 1, c, p, 0] = values[0] * half[p % 2]
                    field[k + 1, c, p, 1] = values[1] * half[p % 2 + 1]
                if outer:
                    put_wide(p, c, tile, values)

    def put_out(k):
        lines = []
        for c in range(3):
            even = field[k + 1, c, 4:12, 0].reshape(64, 128)
            odd = field[k + 1, c, 4:12, 1].reshape(64, 128)
            lines.append(jnp.concatenate([even, odd], axis=1))
        merged = permute(jnp.concatenate(lines, axis=0), pick_t)
        new_basis[k] = merged.reshape(3, 8, 8, 256)

    def zero_edges():
        def clear(ref):
            ref[...] = jnp.zeros(ref.shape, jnp.float32)

        @pl.when(rad == 0)
        def _():
            for e in range(n_exchange):
                clear(field.at[e * DEPTH, :, 4 - up : 4])
                clear(side.at[e, :, :, 4 - up : 4])
            clear(eta.at[:, 0:1])

        @pl.when(rad == n_rad - 1)
        def _():
            for e in range(n_exchange):
                clear(field.at[e * DEPTH, :, 12 : 12 + down])
                clear(side.at[e, :, :, 12 : 12 + down])
            clear(eta.at[:, 3:4])

        @pl.when(lat == 0)
        def _():
            for e in range(n_exchange):
                clear(side.at[e, :, 0])
            clear(eta.at[0])

        @pl.when(lat == n_lat - 1)
        def _():
            for e in range(n_exchange):
                clear(side.at[e, :, 1])
            clear(eta.at[2])

    def send_halo(e, c, which=range(8)):
        each_direction(False, lambda n: halo_copy(e, c, n).start(), which)

    copies[0].wait()
    split_residual(0)
    pack_sides(0, 0, 0)
    pl.semaphore_wait(barrier, 4 + corners)
    each_direction(False, lambda n: eta_copy(n).start())
    send_halo(0, 0)
    for c in range(1, 3):
        split_residual(c)
        pack_sides(0, 0, c)
        send_halo(0, c)
    tell(0)

    zero_edges()
    rows[...] = jnp.zeros(rows.shape, jnp.float32)
    late[...] = jnp.zeros(late.shape, jnp.float32)
    pick_t[...] = (col_id == jnp.where(row_id < 128, 2 * row_id, 2 * row_id - 255)).astype(jnp.float32).astype(jnp.bfloat16)
    for c in range(3):
        widen_own(0, c, range(4, 12))
    copies[4].wait()
    copies[3].wait()
    for m in range(n_prev):
        for c in range(3):

            def store_prev(y, value):
                prev_d[m, c, :, y] = value

            split_y(prev_v[m, c], store_prev)
    for m in range(n_prev + 1):
        dots(m)
    hear(0)
    tell(1)
    each_direction(True, lambda n: eta_copy(n).wait_recv())
    for h in range(4):
        own = eta[1, h]
        beside = jnp.where(sub % 4 < 2, eta[2, h], eta[0, h])
        for half_row, visc in enumerate((
            jnp.where(upper_rows, own, pltpu.roll(beside, 4, 0)),
            jnp.where(upper_rows, pltpu.roll(own, 4, 0), beside),
        )):
            for q, modes in enumerate(WEIGHTS):
                eta_wide[2 * h + half_row, q] = visc * mode_weight(*modes)

    low, high = 4 - up, 12 + down
    for e in range(n_exchange):
        k = e * DEPTH
        final = e == n_exchange - 1

        def component(c, nothing):
            each_direction(True, lambda n: halo_copy(e, c, n).wait_recv())
            widen_own(k, c, list(range(low, 4)) + list(range(12, high)))
            widen_sides(e, c, range(low, high))
            for step in range(DEPTH):
                left = DEPTH - 1 - step
                apply(c, 1 - left, 6 + left, 4 - 2 * left, 11 + left)
                last = step == DEPTH - 1
                advance(
                    k + step, c, range(4 - 2 * left, 12 + left), (0,) if last else (0, 1),
                    not (last and final),
                )
            if final:
                for j in range(k + 1, n_steps + 1):
                    n = n_prev + j
                    sums = tuple(late[j - k - 1, m] for m in range(n + 1))
                    for m, value in enumerate(dot_sums(n, c, sums)):
                        late[j - k - 1, m] = value
            else:
                send_halo(e + 1, c, range(2))
                pack_sides(e + 1, k + DEPTH, c)
                send_halo(e + 1, c, range(2, 8))
            return nothing

        lax.fori_loop(0, 3, component, 0)
        if not final:
            hear(1)
            tell(2)
            for j in range(k + 1, k + DEPTH + 1):
                dots(n_prev + j)
                put_out(j - 1)

    hear(2)
    for j in range(n_steps - DEPTH + 1, n_steps + 1):
        n = n_prev + j
        put_rows(n, [late[j - (n_steps - DEPTH) - 1, m] for m in range(n + 1)])
    ones = jnp.ones((8, 128), jnp.float32)
    local = lax.dot_general(
        ones, rows[...], (((1,), (1,)), ((), ())), precision=HIGHEST, preferred_element_type=jnp.float32
    )
    row_lat[lat] = local[0:1]

    def row_copy(stage, d):
        buffer, me, count = (row_lat, lat, n_lat) if stage == 0 else (row_rad, rad, n_rad)
        peer = lax.rem(me + d, count)
        target = {"lat": peer, "rad": rad} if stage == 0 else {"lat": lat, "rad": peer}
        return pltpu.make_async_remote_copy(
            src_ref=buffer.at[me], dst_ref=buffer.at[me],
            send_sem=gsend_sem.at[stage, d], recv_sem=grecv_sem.at[stage, d],
            device_id=target, device_id_type=MESH,
        )

    for d in sorted(range(1, n_lat), key=lambda d: -min(d, n_lat - d)):
        row_copy(0, d).start()
    for j in range(n_steps - DEPTH + 1, n_steps + 1):
        put_out(j - 1)
    for d in range(1, n_lat):
        row_copy(0, d).wait_recv()
    total = row_lat[0]
    for d in range(1, n_lat):
        total = total + row_lat[d]
    row_rad[rad] = total
    for d in sorted(range(1, n_rad), key=lambda d: -min(d, n_rad - d)):
        row_copy(1, d).start()
    each_direction(False, lambda n: eta_copy(n).wait_send())
    for e in range(n_exchange):
        for c in range(3):
            each_direction(False, lambda n: halo_copy(e, c, n).wait_send())
    for d in range(1, n_lat):
        row_copy(0, d).wait_send()
    for d in range(1, n_rad):
        row_copy(1, d).wait_recv()
    total = row_rad[0]
    for d in range(1, n_rad):
        total = total + row_rad[d]
    gram[...] = total
    for d in range(1, n_rad):
        row_copy(1, d).wait_send()


def leave(dof_count, vectors, sums, new_basis, gram, square, sems):
    away = pltpu.make_async_copy(vectors, new_basis, sems.at[0])
    away.start()
    total = jnp.broadcast_to(sums[...] * (1.0 / dof_count), (8, 128))
    width = square.shape[0]
    for i in range(width):
        line = total if i == 0 else pltpu.roll(total, 128 - i * width, 1)
        square[i : i + 1, :] = line[0:1, :width]
    last = pltpu.make_async_copy(square, gram, sems.at[1])
    last.start()
    away.wait()
    last.wait()


def solution(mesh):
    n_lat = mesh.shape["lat"]
    n_rad = mesh.shape["rad"]

    def on_device(residual, prev_basis, layer_ids, viscosity, shifts):
        n_steps = shifts.shape[0]
        n_prev = prev_basis.shape[0]
        width = n_prev + n_steps + 1
        n_exchange = n_steps // DEPTH
        dof_count = residual.size * n_lat * n_rad
        f32 = jnp.float32
        dma = pltpu.SemaphoreType.DMA
        vectors, sums = pl.pallas_call(
            functools.partial(
                kernel, n_steps, n_prev, viscosity.shape[0], n_rad, n_lat
            ),
            out_shape=(
                jax.ShapeDtypeStruct((n_steps,) + residual.shape, f32),
                jax.ShapeDtypeStruct((1, 128), f32),
            ),
            in_specs=[pl.BlockSpec(memory_space=pltpu.HBM)] * 5,
            out_specs=(
                pl.BlockSpec(memory_space=pltpu.VMEM),
                pl.BlockSpec(memory_space=pltpu.VMEM),
            ),
            scratch_shapes=[
                pltpu.SMEM(viscosity.shape, f32),
                pltpu.SMEM(shifts.shape, f32),
                pltpu.VMEM(residual.shape, f32),
                pltpu.VMEM(prev_basis.shape, f32),
                pltpu.VMEM(layer_ids.shape, jnp.int32),
                pltpu.VMEM((256, 256), jnp.bfloat16),
                pltpu.VMEM((256, 256), jnp.bfloat16),
                pltpu.VMEM((n_steps + 1, 3, 16, 2, 8, 128), f32),
                pltpu.VMEM((n_prev, 3, 8, 2, 8, 128), f32),
                pltpu.VMEM((3, 16, 3, 24, 128), f32),
                pltpu.VMEM((3, 16, 3, 16, 128), f32),
                pltpu.VMEM((n_exchange, 3, 2, 8, 8, 128), f32),
                pltpu.VMEM((n_exchange, 3, 2, 16, 8, 128), f32),
                pltpu.VMEM((3, 4, 8, 128), f32),
                pltpu.VMEM((8, len(WEIGHTS), 8, 128), f32),
                pltpu.VMEM((128, 128), f32),
                pltpu.VMEM((DEPTH, width, 8, 128), f32),
                pltpu.VMEM((n_lat, 1, 128), f32),
                pltpu.VMEM((n_rad, 1, 128), f32),
                pltpu.SemaphoreType.REGULAR((2, 3)),
                dma((5,)),
                dma((n_exchange, 3, 8)),
                dma((n_exchange, 3, 8)),
                dma((8,)),
                dma((8,)),
                dma((2, max(n_lat, n_rad))),
                dma((2, max(n_lat, n_rad))),
            ],
            compiler_params=pltpu.CompilerParams(collective_id=0, has_side_effects=True, vmem_limit_bytes=24 * 2**20),
        )(*(pltpu.with_memory_space_constraint(x, pltpu.HBM) for x in (residual, prev_basis, layer_ids, viscosity, shifts)))

        return pl.pallas_call(
            functools.partial(leave, dof_count),
            out_shape=(
                jax.ShapeDtypeStruct(vectors.shape, f32),
                jax.ShapeDtypeStruct((width, width), f32),
            ),
            in_specs=[pl.BlockSpec(memory_space=pltpu.VMEM)] * 2,
            out_specs=(pl.BlockSpec(memory_space=pltpu.HBM), pl.BlockSpec(memory_space=pltpu.HBM)),
            scratch_shapes=[pltpu.VMEM((width, width), f32), dma((2,))],
            compiler_params=pltpu.CompilerParams(vmem_limit_bytes=2**20),
        )(vectors, sums)

    placed = (P(None, "rad", "lat", None), P(None, None, "rad", "lat", None), P("rad", "lat", None), P(), P())
    return jax.shard_map(
        on_device,
        mesh=mesh,
        in_specs=placed,
        out_specs=(P(None, None, "rad", "lat", None), P()),
        check_vma=False,
    )
```

```python
import functools

import jax
import jax.numpy as jnp
from jax import lax
from jax.experimental import pallas as pl
from jax.experimental.pallas import tpu as pltpu
from jax.sharding import PartitionSpec as P

MESH = pl.DeviceIdType.MESH
HIGHEST = lax.Precision.HIGHEST
DEPTH = 2
MASS = (1.0 / 36.0, 1.0 / 12.0, 1.0 / 45.0)
STIFF = (0.0, 1.0, 4.0 / 3.0)
DIRECTIONS = [(-1, 0), (1, 0), (-1, -1), (-1, 1), (1, -1), (1, 1), (0, -1), (0, 1)]


def mode_weight(i, j, k):
    return (
        STIFF[i] * MASS[j] * MASS[k]
        + MASS[i] * STIFF[j] * MASS[k]
        + MASS[i] * MASS[j] * STIFF[k]
    )


def to_modes(a, b, c):
    ends = a + c
    return ends + (b + b), a - c, ends - b


def from_modes(g0, g1, g2):
    ends = g0 + g2
    return ends + g1, (g0 + g0) - g2, ends - g1


WEIGHTS = [(i, j, l) for i in range(3) for j in range(i, 3) for l in range(j, 3) if l > 0]


def kernel(
    n_steps, n_prev, n_layers, n_rad, n_lat,
    residual, prev_basis, layer_ids, viscosity_in, shifts_in,
    new_basis, gram,
    viscosity, shifts,
    res_v, prev_v, ids_v, pick, pick_t, field, prev_d, wide, parts, pack, side, eta, eta_wide,
    rows, late, row_lat, row_rad,
    known, in_sem, send_sem, recv_sem, esend_sem, erecv_sem, gsend_sem, grecv_sem,
):
    rad = lax.axis_index("rad")
    lat = lax.axis_index("lat")
    n_exchange = n_steps // DEPTH
    up = 2 * DEPTH
    down = 2 * DEPTH - 1

    copies = [
        pltpu.make_async_copy(residual, res_v, in_sem.at[0]),
        pltpu.make_async_copy(layer_ids, ids_v, in_sem.at[1]),
        pltpu.make_async_copy(viscosity_in, viscosity, in_sem.at[3]),
        pltpu.make_async_copy(shifts_in, shifts, in_sem.at[4]),
        pltpu.make_async_copy(prev_basis, prev_v, in_sem.at[2]),
    ]
    for copy in copies:
        copy.start()

    barrier = pltpu.get_barrier_semaphore()

    def here(dr, dl):
        inside = None
        for value, step, count in ((rad, dr, n_rad), (lat, dl, n_lat)):
            if step:
                test = value < count - 1 if step > 0 else value > 0
                inside = test if inside is None else jnp.logical_and(inside, test)
        return inside

    def around(axis, distance):
        if axis == 0:
            return {"lat": lax.rem(lat + distance + n_lat, n_lat), "rad": rad}
        return {"lat": lat, "rad": lax.rem(rad + distance + n_rad, n_rad)}

    corners = 0
    for axis in range(2):
        for d in (-1, 1):
            pl.semaphore_signal(barrier, inc=1, device_id=around(axis, d), device_id_type=MESH)
    for dr in (-1, 1):
        for dl in (-1, 1):
            corners = corners + jnp.where(here(dr, dl), 1, 0)

            @pl.when(here(dr, dl))
            def _():
                pl.semaphore_signal(
                    barrier, inc=1, device_id={"lat": lat + dl, "rad": rad + dr}, device_id_type=MESH
                )

    def tell(r):
        for axis, count in enumerate((n_lat, n_rad)):
            if 2**r % count:
                for d in (-(2**r), 2**r):
                    pl.semaphore_signal(
                        known.at[axis, r], inc=1, device_id=around(axis, d), device_id_type=MESH
                    )

    def hear(r):
        for axis, count in enumerate((n_lat, n_rad)):
            if 2**r % count:
                pl.semaphore_wait(known.at[axis, r], 2)

    sub = lax.broadcasted_iota(jnp.int32, (8, 128), 0)
    lane = lax.broadcasted_iota(jnp.int32, (8, 128), 1)
    upper_rows = sub < 4
    double = [jnp.where(sub % 2 == 0, 1.0, 2.0) * 2.0**q for q in range(3)]
    half = [jnp.where(sub % 2 == 0, 1.0, 0.5) * 0.5**q for q in range(3)]
    square = [jnp.where(sub % 2 == 0, 1.0, 4.0) * 4.0**q for q in range(3)]

    row_id = lax.broadcasted_iota(jnp.int32, (256, 256), 0)
    col_id = lax.broadcasted_iota(jnp.int32, (256, 256), 1)
    pick[...] = (row_id == jnp.where(col_id < 128, 2 * col_id, 2 * col_id - 255)).astype(jnp.float32).astype(jnp.bfloat16)

    def permute(values, table):
        top = values.astype(jnp.bfloat16)
        rest = values - top.astype(jnp.float32)
        middle = rest.astype(jnp.bfloat16)
        last = (rest - middle.astype(jnp.float32)).astype(jnp.bfloat16)
        moved = jnp.dot(
            jnp.concatenate([top, middle, last], axis=0), table[...], preferred_element_type=jnp.float32
        )
        n = values.shape[0]
        return (moved[:n] + moved[n : 2 * n]) + moved[2 * n :]

    def split_y(values, store):
        split = permute(values.reshape(64, 256), pick)
        store(0, split[:, :128].reshape(8, 8, 128))
        store(1, split[:, 128:].reshape(8, 8, 128))

    def split_residual(c):
        def store(y, value):
            field[0, c, 4:12, y] = value

        split_y(res_v[c], store)

    copies[1].wait()
    copies[2].wait()
    layers = []
    for a in range(4):
        ids = ids_v[a]
        values = jnp.zeros(ids.shape, jnp.float32)
        for layer in range(n_layers):
            values = jnp.where(ids == layer, viscosity[layer], values)
        layers.append(values)

    for h in range(2):
        eta[1, 1 + h] = jnp.concatenate(layers[2 * h : 2 * h + 2], axis=0)

    def pack_sides(e, k, c):
        for p in range(8):
            even = field[k, c, 4 + p, 0]
            odd = field[k, c, 4 + p, 1]
            pack[e, c, 0, p] = jnp.where(upper_rows, even, pltpu.roll(odd, 4, 0))
            pack[e, c, 1, p] = jnp.where(upper_rows, pltpu.roll(even, 4, 0), odd)

    def halo_copy(e, c, n, way=1):
        dr, dl = DIRECTIONS[n]
        k = e * DEPTH
        source, target, size = {
            1: (8 - up, 4 - up, up), -1: (0, 12, down), 0: (0, 4, 8)
        }[dr]
        if dl == 0:
            src = field.at[k, c, pl.ds(4 + source, size)]
            dst = field.at[k, c, pl.ds(target, size)]
        else:
            src = pack.at[e, c, 0 if dl < 0 else 1, pl.ds(source, size)]
            dst = side.at[e, c, 1 if dl < 0 else 0, pl.ds(target, size)]
        return pltpu.make_async_remote_copy(
            src_ref=src, dst_ref=dst, send_sem=send_sem.at[e, c, n], recv_sem=recv_sem.at[e, c, n],
            device_id={"lat": lat + way * dl, "rad": rad + way * dr}, device_id_type=MESH,
        )

    def eta_copy(n, way=1):
        dr, dl = DIRECTIONS[n]
        source, target, size = {1: (1, 0, 1), -1: (0, 3, 1), 0: (0, 1, 2)}[dr]
        return pltpu.make_async_remote_copy(
            src_ref=eta.at[1, pl.ds(1 + source, size)],
            dst_ref=eta.at[1 - dl, pl.ds(target, size)],
            send_sem=esend_sem.at[n], recv_sem=erecv_sem.at[n],
            device_id={"lat": lat + way * dl, "rad": rad + way * dr}, device_id_type=MESH,
        )

    def each_direction(receive, act, which=range(8)):
        for n, (dr, dl) in enumerate(DIRECTIONS):
            if n not in which:
                continue
            test = here(-dr, -dl) if receive else here(dr, dl)

            @pl.when(test)
            def _():
                act(n)

    def put_wide(p, c, tile, values):
        for slot, value in enumerate(values):
            wide[c, p, slot, tile * 8 : tile * 8 + 8] = value
            if tile == 0:
                wide[c, p, slot, 16:24] = value

    def widen(p, c, tile, even, odd):
        even = even * double[p % 2]
        odd = odd * double[p % 2 + 1]
        put_wide(p, c, tile, (even, odd, jnp.where(lane < 127, pltpu.roll(even, 127, 1), 0.0)))

    def widen_own(k, c, planes):
        for p in planes:
            widen(p, c, 0, field[k, c, p, 0], field[k, c, p, 1])

    def widen_sides(e, c, planes):
        for p in planes:
            below = side[e, c, 0, p]
            above = side[e, c, 1, p]
            widen(
                p, c, 1,
                jnp.where(upper_rows, above, pltpu.roll(below, 4, 0)),
                jnp.where(upper_rows, pltpu.roll(above, 4, 0), below),
            )

    width = n_prev + n_steps + 1

    def dot_sums(n, c, sums):
        def tile(m, p, y):
            return prev_d[m, c, p, y] if m < n_prev else field[m - n_prev, c, 4 + p, y]

        def body(half, sums):
            sums = list(sums)
            for q in range(4):
                for y in range(2):
                    new = tile(n, half * 4 + q, y)
                    for m in range(n + 1):
                        other = new if m == n else tile(m, half * 4 + q, y)
                        sums[m] = sums[m] + new * other
            return tuple(sums)

        return lax.fori_loop(0, 2, body, sums)

    def put_rows(n, sums):
        for m in range(n + 1):
            total = jnp.sum(sums[m], axis=0, keepdims=True)
            rows[n * width + m : n * width + m + 1] = total
            if m != n:
                rows[m * width + n : m * width + n + 1] = total

    def dots(n):
        zero = jnp.zeros((8, 128), jnp.float32)
        put_rows(n, lax.fori_loop(0, 3, lambda c, sums: dot_sums(n, c, sums), (zero,) * (n + 1)))

    def planes_modes(p, c):
        nodes = [
            [wide[c, p, slot, pl.ds(start, 8, stride=2)] for start in range(3)] for slot in range(3)
        ]
        lines = [to_modes(*nodes[slot]) for slot in range(3)]
        return [to_modes(lines[0][i], lines[1][i], lines[2][i]) for i in range(3)]

    def put_plane(p, c, modes):
        lines = [from_modes(*modes[i]) for i in range(3)]
        for slot in range(3):
            low, mid, high = from_modes(lines[0][slot], lines[1][slot], lines[2][slot])
            parts[c, p, slot, pl.ds(0, 8, stride=2)] = low + pltpu.roll(high, 1, 0)
            parts[c, p, slot, pl.ds(1, 8, stride=2)] = mid

    def apply(c, first, last, low_plane, high_plane):
        below = planes_modes(2 * first, c)
        carried = None
        for a in range(first, last):
            middle = planes_modes(2 * a + 1, c)
            above = planes_modes(2 * a + 2, c)
            at_low = [[None] * 3 for _ in range(3)]
            at_mid = [[None] * 3 for _ in range(3)]
            at_high = [[None] * 3 for _ in range(3)]
            for i in range(3):
                for j in range(3):
                    m = to_modes(below[i][j], middle[i][j], above[i][j])
                    g = [
                        None if i + j + l == 0 else m[l] * eta_wide[a, WEIGHTS.index(tuple(sorted((i, j, l))))]
                        for l in range(3)
                    ]
                    if g[0] is None:
                        out = (g[2] + g[1], -g[2], g[2] - g[1])
                    else:
                        out = from_modes(*g)
                    at_low[i][j] = out[0] if carried is None else out[0] + carried[i][j]
                    at_mid[i][j] = out[1]
                    at_high[i][j] = out[2]
            if low_plane <= 2 * a <= high_plane:
                put_plane(2 * a, c, at_low)
            if low_plane <= 2 * a + 1 <= high_plane:
                put_plane(2 * a + 1, c, at_mid)
            carried = at_high
            below = above

    keep_rad = jnp.where(rad == n_rad - 1, 0.0, 1.0)
    keep_lat = jnp.where(jnp.logical_and(upper_rows, lat == n_lat - 1), 0.0, 1.0)

    def advance(k, c, planes, tiles, outer):
        shift = shifts[k]
        for p in planes:
            for tile in tiles:
                at = slice(tile * 8, tile * 8 + 8)
                low = parts[c, p, 0, at]
                high = parts[c, p, 2, at]
                moved = jnp.where(lane > 0, pltpu.roll(high, 1, 1), 0.0)
                even = square[p % 2] * (low + moved) - shift * wide[c, p, 0, at]
                odd = square[p % 2 + 1] * parts[c, p, 1, at] - shift * wide[c, p, 1, at]
                values = [even, odd]
                if outer:
                    after = jnp.where(lane < 127, pltpu.roll(low, 127, 1) + high, 0.0)
                    values.append(square[p % 2] * after - shift * wide[c, p, 2, at])
                if p >= 12:
                    values = [value * keep_rad for value in values]
                if tile == 1:
                    values = [value * keep_lat for value in values]
                if tile == 0 and 4 <= p < 12:
                    field[k + 1, c, p, 0] = values[0] * half[p % 2]
                    field[k + 1, c, p, 1] = values[1] * half[p % 2 + 1]
                if outer:
                    put_wide(p, c, tile, values)

    def put_out(k):
        lines = []
        for c in range(3):
            even = field[k + 1, c, 4:12, 0].reshape(64, 128)
            odd = field[k + 1, c, 4:12, 1].reshape(64, 128)
            lines.append(jnp.concatenate([even, odd], axis=1))
        merged = permute(jnp.concatenate(lines, axis=0), pick_t)
        new_basis[k] = merged.reshape(3, 8, 8, 256)

    def zero_edges():
        def clear(ref):
            ref[...] = jnp.zeros(ref.shape, jnp.float32)

        @pl.when(rad == 0)
        def _():
            for e in range(n_exchange):
                clear(field.at[e * DEPTH, :, 4 - up : 4])
                clear(side.at[e, :, :, 4 - up : 4])
            clear(eta.at[:, 0:1])

        @pl.when(rad == n_rad - 1)
        def _():
            for e in range(n_exchange):
                clear(field.at[e * DEPTH, :, 12 : 12 + down])
                clear(side.at[e, :, :, 12 : 12 + down])
            clear(eta.at[:, 3:4])

        @pl.when(lat == 0)
        def _():
            for e in range(n_exchange):
                clear(side.at[e, :, 0])
            clear(eta.at[0])

        @pl.when(lat == n_lat - 1)
        def _():
            for e in range(n_exchange):
                clear(side.at[e, :, 1])
            clear(eta.at[2])

    def send_halo(e, c, which=range(8)):
        each_direction(False, lambda n: halo_copy(e, c, n).start(), which)

    copies[0].wait()
    split_residual(0)
    pack_sides(0, 0, 0)
    pl.semaphore_wait(barrier, 4 + corners)
    each_direction(False, lambda n: eta_copy(n).start())
    send_halo(0, 0)
    for c in range(1, 3):
        split_residual(c)
        pack_sides(0, 0, c)
        send_halo(0, c)
    tell(0)

    zero_edges()
    rows[...] = jnp.zeros(rows.shape, jnp.float32)
    late[...] = jnp.zeros(late.shape, jnp.float32)
    pick_t[...] = (col_id == jnp.where(row_id < 128, 2 * row_id, 2 * row_id - 255)).astype(jnp.float32).astype(jnp.bfloat16)
    for c in range(3):
        widen_own(0, c, range(4, 12))
    copies[4].wait()
    copies[3].wait()
    for m in range(n_prev):
        for c in range(3):

            def store_prev(y, value):
                prev_d[m, c, :, y] = value

            split_y(prev_v[m, c], store_prev)
    for m in range(n_prev + 1):
        dots(m)
    hear(0)
    tell(1)
    each_direction(True, lambda n: eta_copy(n, -1).wait_recv())
    for h in range(4):
        own = eta[1, h]
        beside = jnp.where(sub % 4 < 2, eta[2, h], eta[0, h])
        for half_row, visc in enumerate((
            jnp.where(upper_rows, own, pltpu.roll(beside, 4, 0)),
            jnp.where(upper_rows, pltpu.roll(own, 4, 0), beside),
        )):
            for q, modes in enumerate(WEIGHTS):
                eta_wide[2 * h + half_row, q] = visc * mode_weight(*modes)

    low, high = 4 - up, 12 + down
    for e in range(n_exchange):
        k = e * DEPTH
        final = e == n_exchange - 1

        def component(c, nothing):
            each_direction(True, lambda n: halo_copy(e, c, n, -1).wait_recv())
            widen_own(k, c, list(range(low, 4)) + list(range(12, high)))
            widen_sides(e, c, range(low, high))
            for step in range(DEPTH):
                left = DEPTH - 1 - step
                apply(c, 1 - left, 6 + left, 4 - 2 * left, 11 + left)
                last = step == DEPTH - 1
                advance(
                    k + step, c, range(4 - 2 * left, 12 + left), (0,) if last else (0, 1),
                    not (last and final),
                )
            if final:
                for j in range(k + 1, n_steps + 1):
                    n = n_prev + j
                    sums = tuple(late[j - k - 1, m] for m in range(n + 1))
                    for m, value in enumerate(dot_sums(n, c, sums)):
                        late[j - k - 1, m] = value
            else:
                send_halo(e + 1, c, range(2))
                pack_sides(e + 1, k + DEPTH, c)
                send_halo(e + 1, c, range(2, 8))
            return nothing

        lax.fori_loop(0, 3, component, 0)
        if not final:
            hear(1)
            tell(2)
            for j in range(k + 1, k + DEPTH + 1):
                dots(n_prev + j)
                put_out(j - 1)

    hear(2)
    for j in range(n_steps - DEPTH + 1, n_steps + 1):
        n = n_prev + j
        put_rows(n, [late[j - (n_steps - DEPTH) - 1, m] for m in range(n + 1)])
    ones = jnp.ones((8, 128), jnp.float32)
    local = lax.dot_general(
        ones, rows[...], (((1,), (1,)), ((), ())), precision=HIGHEST, preferred_element_type=jnp.float32
    )
    row_lat[lat] = local[0:1]

    def row_copy(stage, d):
        buffer, me, count = (row_lat, lat, n_lat) if stage == 0 else (row_rad, rad, n_rad)
        peer = lax.rem(me + d, count)
        target = {"lat": peer, "rad": rad} if stage == 0 else {"lat": lat, "rad": peer}
        return pltpu.make_async_remote_copy(
            src_ref=buffer.at[me], dst_ref=buffer.at[me],
            send_sem=gsend_sem.at[stage, d], recv_sem=grecv_sem.at[stage, d],
            device_id=target, device_id_type=MESH,
        )

    for d in sorted(range(1, n_lat), key=lambda d: -min(d, n_lat - d)):
        row_copy(0, d).start()
    for j in range(n_steps - DEPTH + 1, n_steps + 1):
        put_out(j - 1)
    for d in range(1, n_lat):
        row_copy(0, d).wait_recv()
    total = row_lat[0]
    for d in range(1, n_lat):
        total = total + row_lat[d]
    row_rad[rad] = total
    for d in sorted(range(1, n_rad), key=lambda d: -min(d, n_rad - d)):
        row_copy(1, d).start()
    each_direction(False, lambda n: eta_copy(n).wait_send())
    for e in range(n_exchange):
        for c in range(3):
            each_direction(False, lambda n: halo_copy(e, c, n).wait_send())
    for d in range(1, n_lat):
        row_copy(0, d).wait_send()
    for d in range(1, n_rad):
        row_copy(1, d).wait_recv()
    total = row_rad[0]
    for d in range(1, n_rad):
        total = total + row_rad[d]
    gram[...] = total
    for d in range(1, n_rad):
        row_copy(1, d).wait_send()


def leave(dof_count, vectors, sums, new_basis, gram, square, sems):
    away = pltpu.make_async_copy(vectors, new_basis, sems.at[0])
    away.start()
    total = jnp.broadcast_to(sums[...] * (1.0 / dof_count), (8, 128))
    width = square.shape[0]
    for i in range(width):
        line = total if i == 0 else pltpu.roll(total, 128 - i * width, 1)
        square[i : i + 1, :] = line[0:1, :width]
    last = pltpu.make_async_copy(square, gram, sems.at[1])
    last.start()
    away.wait()
    last.wait()


def solution(mesh):
    n_lat = mesh.shape["lat"]
    n_rad = mesh.shape["rad"]

    def on_device(residual, prev_basis, layer_ids, viscosity, shifts):
        n_steps = shifts.shape[0]
        n_prev = prev_basis.shape[0]
        width = n_prev + n_steps + 1
        n_exchange = n_steps // DEPTH
        dof_count = residual.size * n_lat * n_rad
        f32 = jnp.float32
        dma = pltpu.SemaphoreType.DMA
        vectors, sums = pl.pallas_call(
            functools.partial(
                kernel, n_steps, n_prev, viscosity.shape[0], n_rad, n_lat
            ),
            out_shape=(
                jax.ShapeDtypeStruct((n_steps,) + residual.shape, f32),
                jax.ShapeDtypeStruct((1, 128), f32),
            ),
            in_specs=[pl.BlockSpec(memory_space=pltpu.HBM)] * 5,
            out_specs=(
                pl.BlockSpec(memory_space=pltpu.VMEM),
                pl.BlockSpec(memory_space=pltpu.VMEM),
            ),
            scratch_shapes=[
                pltpu.SMEM(viscosity.shape, f32),
                pltpu.SMEM(shifts.shape, f32),
                pltpu.VMEM(residual.shape, f32),
                pltpu.VMEM(prev_basis.shape, f32),
                pltpu.VMEM(layer_ids.shape, jnp.int32),
                pltpu.VMEM((256, 256), jnp.bfloat16),
                pltpu.VMEM((256, 256), jnp.bfloat16),
                pltpu.VMEM((n_steps + 1, 3, 16, 2, 8, 128), f32),
                pltpu.VMEM((n_prev, 3, 8, 2, 8, 128), f32),
                pltpu.VMEM((3, 16, 3, 24, 128), f32),
                pltpu.VMEM((3, 16, 3, 16, 128), f32),
                pltpu.VMEM((n_exchange, 3, 2, 8, 8, 128), f32),
                pltpu.VMEM((n_exchange, 3, 2, 16, 8, 128), f32),
                pltpu.VMEM((3, 4, 8, 128), f32),
                pltpu.VMEM((8, len(WEIGHTS), 8, 128), f32),
                pltpu.VMEM((128, 128), f32),
                pltpu.VMEM((DEPTH, width, 8, 128), f32),
                pltpu.VMEM((n_lat, 1, 128), f32),
                pltpu.VMEM((n_rad, 1, 128), f32),
                pltpu.SemaphoreType.REGULAR((2, 3)),
                dma((5,)),
                dma((n_exchange, 3, 8)),
                dma((n_exchange, 3, 8)),
                dma((8,)),
                dma((8,)),
                dma((2, max(n_lat, n_rad))),
                dma((2, max(n_lat, n_rad))),
            ],
            compiler_params=pltpu.CompilerParams(collective_id=0, has_side_effects=True, vmem_limit_bytes=24 * 2**20),
        )(*(pltpu.with_memory_space_constraint(x, pltpu.HBM) for x in (residual, prev_basis, layer_ids, viscosity, shifts)))

        return pl.pallas_call(
            functools.partial(leave, dof_count),
            out_shape=(
                jax.ShapeDtypeStruct(vectors.shape, f32),
                jax.ShapeDtypeStruct((width, width), f32),
            ),
            in_specs=[pl.BlockSpec(memory_space=pltpu.VMEM)] * 2,
            out_specs=(pl.BlockSpec(memory_space=pltpu.HBM), pl.BlockSpec(memory_space=pltpu.HBM)),
            scratch_shapes=[pltpu.VMEM((width, width), f32), dma((2,))],
            compiler_params=pltpu.CompilerParams(vmem_limit_bytes=2**20),
        )(vectors, sums)

    placed = (P(None, "rad", "lat", None), P(None, None, "rad", "lat", None), P("rad", "lat", None), P(), P())
    return jax.shard_map(
        on_device,
        mesh=mesh,
        in_specs=placed,
        out_specs=(P(None, None, "rad", "lat", None), P()),
        check_vma=False,
    )
```
